256 devices in a mesh: mz: 64 (over z, x, core), rep: 4 (over y).
Axes of the slice: x: 4, y: 4, z: 8, core: 2. Of those that a mesh axis runs over, the one named last changes fastest.
Arguments:
- spectra: bfloat16 [1048576, 512], P(('mz', 'rep')), may hold values from -6 to 6
- reach_back: int32 [1048576], P(('mz', 'rep')), may hold values from 0 to 256
- reach_ahead: int32 [1048576], P(('mz', 'rep')), may hold values from 0 to 256
- live: int32 [256], P(('mz', 'rep')), may hold values from 1024 to 4096, as said below
- cluster_ids: int32 [1048576], P(('mz', 'rep')), may hold values from 0 to 131071, as said below
Outputs:
- cluster_vectors: float32 [131072, 512], P(('mz', 'rep'))
The draws below stay inside these ranges and needn't reach their ends.
Inputs may be any that keep to these rules, and one draw needn't show every extreme that they name: Device d holds slots d * 4096 to (d + 1) * 4096 - 1, of which the first live[d] are occupied; at least one device is full. `cluster_ids`: cluster k is owned by m/z range k div (512 * 4). Range d is held by devices d * 4 to d * 4 + 4 - 1 in order of rising m/z; a spectrum on the first of them belongs to a cluster owned by range d - 1 or d, one on the last of them to a cluster owned by range d or d + 1, and one on any other to a cluster owned by range d.
All inputs are finite; a program needn't handle non-finite values.
Results may differ from the reference program's by a relative error of at most 0.0046.
Values may be sent and summed in bfloat16 or wider, within the bound.
No kernel may reach another device: no remote copies, remote signals or barrier semaphores. Data moves between devices by JAX's collectives and lax.ppermute only.
A program may use at most 128 MiB of HBM per device.

```python
import jax
import jax.numpy as jnp
from jax import lax

DIM = 512
BLOCK = 256
ROWS_DEV = 4096
CL_DEV = 512
NSPEC = 1048576
NCLUST = 131072
N_MZ = 64
N_REP = 4


def draw_live(key, part):
    count = N_MZ * N_REP
    values = jax.random.randint(key, (count,), ROWS_DEV // 4, ROWS_DEV + 1)
    full = jax.random.randint(jax.random.fold_in(key, 7), (), 0, count)
    return jnp.where(jnp.arange(count) == full, ROWS_DEV, values).astype(jnp.int32)


def draw_cluster_ids(key, part):
    total_rows = ROWS_DEV * N_MZ * N_REP
    position = jnp.arange(total_rows, dtype=jnp.int32)
    range_index = position // (ROWS_DEV * N_REP)
    rep_index = position // ROWS_DEV % N_REP
    coin = jax.random.randint(jax.random.fold_in(key, 3), (total_rows,), 0, 4)
    away = coin != 0
    step = jnp.where((rep_index == 0) & away, -1, jnp.where((rep_index == N_REP - 1) & away, 1, 0))
    owner = jnp.clip(range_index + step, 0, N_MZ - 1)
    inner = jax.random.randint(jax.random.fold_in(key, 5), (total_rows,), 0, CL_DEV * N_REP)
    return (owner * (CL_DEV * N_REP) + inner).astype(jnp.int32)


def plant(result, key, low, largest):
    shape = result.shape
    spot = [jax.random.randint(jax.random.fold_in(key, axis), (), 0, shape[axis]) for axis in range(len(shape))]
    result = result.at[tuple(spot)].set(low)
    longest = shape.index(max(shape))
    spot[longest] = (spot[longest] + 1) % shape[longest]
    return result.at[tuple(spot)].set(largest)


def block_scale(stream_key, shape, cuts, least, high):
    gain, own = 1.0, jax.random.fold_in(stream_key, 6)
    for dim, parts in cuts:
        draws = jnp.exp(jax.random.uniform(jax.random.fold_in(own, dim), (parts,), jnp.float32, least / len(cuts), high / len(cuts)))
        gain = gain * jnp.repeat(draws, shape[dim] // parts).reshape([-1 if axis == dim else 1 for axis in range(len(shape))])
    return gain


def centred(stream_key, shape, scale, bound, cuts=(), held_as=jnp.bfloat16):
    level = block_scale(stream_key, shape, cuts, -0.22, 0.18) if cuts else 1.0
    array = jax.random.normal(stream_key, shape, jnp.float32) * scale * level
    return jnp.minimum(jnp.maximum(array, -bound), bound).astype(held_as)


def setup_inputs(seed: int = 0) -> dict:
    key_list = jax.random.split(jax.random.key(seed), 6)
    return {
        "spectra": centred(key_list[0], (NSPEC, DIM), 1.0, 6.0, ((0, 256),)),
        "reach_back": plant(jax.random.randint(key_list[1], (NSPEC,), 0, BLOCK + 1), jax.random.fold_in(key_list[1], 1), 0, BLOCK).astype(jnp.int32),
        "reach_ahead": plant(jax.random.randint(key_list[2], (NSPEC,), 0, BLOCK + 1), jax.random.fold_in(key_list[2], 1), 0, BLOCK).astype(jnp.int32),
        "live": draw_live(jax.random.fold_in(key_list[5], 71), 0),
        "cluster_ids": draw_cluster_ids(jax.random.fold_in(key_list[5], 71), 0),
    }


sharpness = 3.0

def rows_block(queries, query_pos, back, ahead, keys, key_flags, key_start):
    scores = lax.dot_general(queries, keys, (((1,), (1,)), ((), ())), preferred_element_type=jnp.float32)
    key_pos = key_start + jnp.arange(keys.shape[0], dtype=jnp.int32)
    offset = key_pos[None, :] - query_pos[:, None]
    inside = (offset >= -back[:, None]) & (offset <= ahead[:, None]) & (key_flags[None, :] > 0)
    keep = inside | (offset == 0)
    weight = jnp.where(keep, jnp.exp(sharpness * (scores - 1.0)), jnp.float32(0.0))
    total = lax.optimization_barrier(jnp.sum(weight, axis=1, keepdims=True))
    mixed = jnp.dot(weight.astype(jnp.bfloat16), keys, preferred_element_type=jnp.float32)
    return (mixed / total).astype(jnp.bfloat16)

def reference(spectra, reach_back, reach_ahead, live, cluster_ids):
    total_rows = spectra.shape[0]
    values = spectra.astype(jnp.float32)
    unit = (values / jnp.sqrt(lax.optimization_barrier(jnp.sum(values * values, axis=1, keepdims=True)) + 1e-06)).astype(jnp.bfloat16)
    position = jnp.arange(total_rows, dtype=jnp.int32)
    present = position % ROWS_DEV < live[position // ROWS_DEV]
    flags = present.astype(jnp.bfloat16)
    padded_unit = jnp.pad(unit, ((BLOCK, BLOCK), (0, 0)))
    padded_flags = jnp.pad(flags, (BLOCK, BLOCK))

    def one_block(index):
        start = (index * BLOCK).astype(jnp.int32)
        queries = lax.dynamic_slice_in_dim(unit, start, BLOCK, 0)
        back = lax.dynamic_slice_in_dim(reach_back, start, BLOCK, 0)
        ahead = lax.dynamic_slice_in_dim(reach_ahead, start, BLOCK, 0)
        keys = lax.dynamic_slice_in_dim(padded_unit, start, 3 * BLOCK, 0)
        key_flags = lax.dynamic_slice_in_dim(padded_flags, start, 3 * BLOCK, 0)
        query_pos = start + jnp.arange(BLOCK, dtype=jnp.int32)
        return rows_block(queries, query_pos, back, ahead, keys, key_flags, start - BLOCK)
    blocks = lax.map(one_block, jnp.arange(total_rows // BLOCK, dtype=jnp.int32))
    consensus = blocks.reshape(total_rows, DIM)
    kept = consensus.astype(jnp.float32) * present.astype(jnp.float32)[:, None]
    sums = jax.ops.segment_sum(kept, cluster_ids, num_segments=NCLUST)
    scale = jnp.sqrt(lax.optimization_barrier(jnp.mean(sums * sums, axis=1, keepdims=True)) + 1e-06)
    return sums / scale
```

```python
import functools

import jax
import jax.numpy as jnp
from jax import lax
from jax.experimental import pallas as pl
from jax.experimental.pallas import tpu as pltpu
from jax.sharding import PartitionSpec as P

DIM = 512
BLOCK = 256
CL_DEV = 512
ROWS = 4096
NBLK = ROWS // BLOCK
HALO = BLOCK + 16
FAR = -(1 << 24)
SCALE = 3.0 * 1.4426950408889634
f32, bf16, i32 = jnp.float32, jnp.bfloat16, jnp.int32
NT = (((1,), (1,)), ((), ()))


def unit_rows(block):
    values = block.astype(f32)
    square = jnp.sum(values * values, axis=1, keepdims=True)
    return (values * lax.rsqrt(square + 1e-06)).astype(bf16)


def transposed(unit):
    return jnp.transpose(unit)


def attend(query, back, ahead, cap, keys, keys_t, low_cap, high_cap):
    at = lax.broadcasted_iota(i32, (1, BLOCK), 1) + BLOCK
    low = at - back
    high = at + ahead
    own = jnp.minimum(high, cap - 1)
    total = None
    mixed = None
    for k in range(3):
        scores = lax.dot_general(keys[k], query, NT, preferred_element_type=f32)
        slot = lax.broadcasted_iota(i32, (BLOCK, BLOCK), 0) + k * BLOCK
        if k == 0:
            keep = slot >= low
            if low_cap is not None:
                keep = keep & (slot < low_cap)
        elif k == 1:
            keep = ((slot >= low) & (slot <= own)) | (slot == at)
        elif high_cap is None:
            keep = slot <= own
        else:
            keep = slot <= jnp.minimum(high, high_cap - 1)
        weight = jnp.where(keep, jnp.exp2(scores * SCALE - SCALE), 0.0)
        part = jnp.sum(weight, axis=0, keepdims=True)
        term = jnp.dot(keys_t[k], weight.astype(bf16), preferred_element_type=f32)
        total = part if total is None else total + part
        mixed = term if mixed is None else mixed + term
    return (mixed * (1.0 / total)).astype(bf16)


def interior_kernel(live_ref, back_ref, ahead_ref, spectra_ref, out_ref, unit_ref, unit_t_ref):
    def prepare(index):
        start = pl.multiple_of(index * BLOCK, BLOCK)
        unit = unit_rows(spectra_ref[pl.ds(start, BLOCK), :])
        unit_ref[index] = unit
        unit_t_ref[index] = transposed(unit)

    for index in range(3):
        prepare(index)
    live = live_ref[0]

    def step(index, _):
        start = pl.multiple_of(index * BLOCK, BLOCK)
        lanes = pl.ds(start, BLOCK)
        prepare(jnp.minimum(index + 2, NBLK - 1))
        out_ref[:, pl.ds(pl.multiple_of(start - BLOCK, BLOCK), BLOCK)] = attend(
            unit_ref[index],
            back_ref[:, lanes],
            ahead_ref[:, lanes],
            live - (start - BLOCK),
            [unit_ref[index + k] for k in (-1, 0, 1)],
            [unit_t_ref[index + k] for k in (-1, 0, 1)],
            None,
            None,
        )
        return 0

    lax.fori_loop(1, NBLK - 1, step, 0)


def edges_kernel(live_ref, back_ref, ahead_ref, spectra_ref, below_ref, above_ref, out_ref):
    live = live_ref[0]

    def count(ref):
        digits = ref[BLOCK : BLOCK + 8, :BLOCK].astype(f32)
        return (digits[0:1] * 64.0 + digits[1:2]).astype(i32)

    def unit(block):
        return unit_rows(spectra_ref[block * BLOCK : (block + 1) * BLOCK, :])

    keys = [unit_rows(below_ref[:BLOCK, :]), unit(0), unit(1)]
    out_ref[:, :BLOCK] = attend(
        keys[1], back_ref[:, :BLOCK], ahead_ref[:, :BLOCK], live + BLOCK, keys,
        [transposed(k) for k in keys], count(below_ref) - (ROWS - BLOCK), None,
    )
    keys = [unit(NBLK - 2), unit(NBLK - 1), unit_rows(above_ref[:BLOCK, :])]
    out_ref[:, BLOCK:] = attend(
        keys[1], back_ref[:, ROWS - BLOCK :], ahead_ref[:, ROWS - BLOCK :],
        live - (ROWS - 2 * BLOCK), keys, [transposed(k) for k in keys],
        None, count(above_ref) + 2 * BLOCK,
    )


INNER = ROWS - 2 * BLOCK
CHUNK = INNER // 4


def added(first, live, ids_ref, rows, start):
    width = rows.shape[1]
    slot = lax.broadcasted_iota(i32, (1, width), 1) + start
    wanted = jnp.where(slot < live, ids_ref[:, start : start + width] - first, FAR)
    hot = lax.broadcasted_iota(i32, (CL_DEV, width), 0) == wanted
    hot = jnp.where(hot, 1.0, 0.0).astype(bf16)
    return lax.dot_general(hot, rows, NT, preferred_element_type=f32)


def sums_kernel(turns, away, rep_count, live_ref, ids_ref, inner_ref, edge_ref, *outs):
    rep = lax.axis_index("rep")
    band = lax.axis_index("mz")
    per_range = CL_DEV * rep_count
    if away:
        band = band + jnp.where(rep == 0, -1, 1)

    def work():
        live = live_ref[0]
        for turn, out_ref in zip(turns, outs):
            owner = lax.rem(rep + turn, rep_count)
            first = band * per_range + owner * CL_DEV

            acc = added(first, live, ids_ref, edge_ref[:, :BLOCK], 0)
            acc = acc + added(first, live, ids_ref, edge_ref[:, BLOCK:], ROWS - BLOCK)
            for start in range(0, INNER, CHUNK):
                acc = acc + added(first, live, ids_ref, inner_ref[:, start : start + CHUNK], start + BLOCK)
            out_ref[...] = acc.astype(out_ref.dtype)

    if away:
        pl.when((rep == 0) | (rep == rep_count - 1))(work)
    else:
        work()


def finish_kernel(own_ref, *rest):
    out_ref = rest[-1]
    owned = own_ref[...]
    for ref in rest[:-1]:
        owned = owned + ref[...].astype(f32)
    mean = jnp.sum(owned * owned, axis=1, keepdims=True) * (1.0 / DIM)
    out_ref[...] = owned / jnp.sqrt(mean + 1e-06)


VMEM = pl.BlockSpec(memory_space=pltpu.VMEM)
SMEM = pl.BlockSpec(memory_space=pltpu.SMEM)
LIMIT = 40 * 1024 * 1024


def call(kernel, name, inputs, out_shape, flops, scratch=(), limit=LIMIT):
    one = not isinstance(out_shape, (list, tuple))
    in_specs = [SMEM if x.dtype == i32 and x.size < 64 else VMEM for x in inputs]
    moved = sum(x.size * x.dtype.itemsize for x in inputs)
    return pl.pallas_call(
        kernel,
        out_shape=out_shape,
        in_specs=in_specs,
        out_specs=VMEM if one else [VMEM] * len(out_shape),
        scratch_shapes=list(scratch),
        name=name,
        cost_estimate=pl.CostEstimate(flops=flops, bytes_accessed=moved, transcendentals=0),
        compiler_params=pltpu.CompilerParams(vmem_limit_bytes=limit),
    )(*inputs)


def shape(rows, columns, dtype):
    return jax.ShapeDtypeStruct((rows, columns), dtype)


def shards(spectra, reach_back, reach_ahead, live, cluster_ids):
    bands, reps = lax.axis_size("mz"), lax.axis_size("rep")
    every = bands * reps
    both = ("mz", "rep")

    def sum_blocks(turns, away, dtype, name):
        return call(
            functools.partial(sums_kernel, turns, away, reps), name,
            [live, ids, inner, edge], [shape(CL_DEV, DIM, dtype)] * len(turns),
            2 * CL_DEV * ROWS * DIM * len(turns),
        )

    tail = jnp.concatenate(
        [jnp.full((1, DIM), live[0] // 64), jnp.full((15, DIM), live[0] % 64)], axis=0
    ).astype(bf16)
    from_below = lax.ppermute(
        jnp.concatenate([spectra[ROWS - BLOCK :], tail]), both, [(i, i + 1) for i in range(every - 1)]
    )
    from_above = lax.ppermute(
        jnp.concatenate([spectra[:BLOCK], tail]), both, [(i + 1, i) for i in range(every - 1)]
    )
    back, ahead, ids = (x.reshape(1, ROWS) for x in (reach_back, reach_ahead, cluster_ids))
    per_block = 4 * BLOCK * 3 * BLOCK * DIM
    inner = call(
        interior_kernel, "interior", [live, back, ahead, spectra], shape(DIM, INNER, bf16), per_block * (NBLK - 2),
        [pltpu.VMEM((NBLK, BLOCK, DIM), bf16), pltpu.VMEM((NBLK, DIM, BLOCK), bf16)],
    )
    edge = call(
        edges_kernel, "edges", [live, back, ahead, spectra, from_below, from_above],
        shape(DIM, 2 * BLOCK, bf16), 2 * per_block,
    )

    away_pairs = [(d * reps, (d - 1) * reps) for d in range(1, bands)]
    away_pairs += [(d * reps + reps - 1, (d + 1) * reps + reps - 1) for d in range(bands - 1)]
    moved = {}
    for turn in (2, 1, 3, 0):
        (block,) = sum_blocks((turn,), True, bf16, f"away{turn}")
        moved[turn] = lax.ppermute(block, both, away_pairs)
    up = [(i, (i + 1) % reps) for i in range(reps)]
    down = [(b, a) for a, b in up]
    own = {}
    (own[2],) = sum_blocks((2,), False, f32, "own2")
    far = (own[2] + moved[2].astype(f32)).astype(bf16)
    half = CL_DEV // 2
    low_half = lax.ppermute(far[:half], "rep", up)
    high_half = lax.ppermute(far[half:], "rep", down)
    own[1], own[3] = sum_blocks((1, 3), False, f32, "own13")
    (own[0],) = sum_blocks((0,), False, f32, "own0")
    next_up = own[1] + moved[1].astype(f32)
    next_up = jnp.concatenate([next_up[:half] + low_half.astype(f32), next_up[half:]]).astype(bf16)
    next_down = own[3] + moved[3].astype(f32)
    next_down = jnp.concatenate([next_down[:half], next_down[half:] + high_half.astype(f32)]).astype(bf16)
    got_up = lax.ppermute(next_up, "rep", up)
    got_down = lax.ppermute(next_down, "rep", down)
    return call(finish_kernel, "finish", [own[0], moved[0], got_up, got_down], shape(CL_DEV, DIM, f32), 1 << 20)


def solution(mesh):
    rows = P(("mz", "rep"))
    return jax.shard_map(
        shards,
        mesh=mesh,
        in_specs=(P(("mz", "rep"), None), rows, rows, rows, rows),
        out_specs=P(("mz", "rep"), None),
        check_vma=False,
    )
```

```python
import functools

import jax
import jax.numpy as jnp
from jax import lax
from jax.experimental import pallas as pl
from jax.experimental.pallas import tpu as pltpu
from jax.sharding import PartitionSpec as P


DIM = 512
BLOCK = 256
CL_DEV = 512
ROWS = 4096
NBLK = ROWS // BLOCK
HALO = BLOCK + 16
FAR = -(1 << 24)
SCALE = 3.0 * 1.4426950408889634
f32, bf16, i32 = jnp.float32, jnp.bfloat16, jnp.int32
NT = (((1,), (1,)), ((), ()))


def unit_rows(block):
    values = block.astype(f32)
    square = jnp.sum(values * values, axis=1, keepdims=True)
    return (values * lax.rsqrt(square + 1e-06)).astype(bf16)


def transposed(unit):
    return jnp.transpose(unit)


def attend(query, back, ahead, cap, keys, keys_t, low_cap, high_cap):
    at = lax.broadcasted_iota(i32, (1, BLOCK), 1) + BLOCK
    low = at - back
    high = at + ahead
    own = jnp.minimum(high, cap - 1)
    total = None
    mixed = None
    for k in range(3):
        scores = lax.dot_general(keys[k], query, NT, preferred_element_type=f32)
        slot = lax.broadcasted_iota(i32, (BLOCK, BLOCK), 0) + k * BLOCK
        if k == 0:
            keep = slot >= low
            if low_cap is not None:
                keep = keep & (slot < low_cap)
        elif k == 1:
            keep = ((slot >= low) & (slot <= own)) | (slot == at)
        elif high_cap is None:
            keep = slot <= own
        else:
            keep = slot <= jnp.minimum(high, high_cap - 1)
        weight = jnp.where(keep, jnp.exp2(scores * SCALE - SCALE), 0.0)
        part = jnp.sum(weight, axis=0, keepdims=True)
        term = jnp.dot(keys_t[k], weight.astype(bf16), preferred_element_type=f32)
        total = part if total is None else total + part
        mixed = term if mixed is None else mixed + term
    return (mixed * (1.0 / total)).astype(bf16)


def pack_kernel(live_ref, first_ref, last_ref, low_ref, high_ref):
    live = live_ref[0]
    row = lax.broadcasted_iota(i32, (HALO - BLOCK, DIM), 0)
    digits = jnp.where(row == 0, live >> 6, live & 63).astype(f32).astype(bf16)
    for source, ref in ((first_ref, low_ref), (last_ref, high_ref)):
        ref[:BLOCK, :] = source[...]
        ref[BLOCK:, :] = digits


def interior_kernel(
    live_ref, back_ref, ahead_ref, rows_ref, out_ref,
    unit_ref, unit_t_ref, score_a, score_b, weight_a, weight_b,
):
    live = live_ref[0]

    def block(index):
        return pl.ds(pl.multiple_of(index * BLOCK, BLOCK), BLOCK)

    def prepare(index):
        unit = unit_rows(rows_ref[block(index), :])
        unit_ref[block(index), :] = unit
        unit_t_ref[:, block(index)] = transposed(unit)

    def score(index, score_ref):
        query = unit_ref[block(index), :]
        for k in range(3):
            score_ref[k * BLOCK : (k + 1) * BLOCK, :] = lax.dot_general(
                unit_ref[block(index + k - 1), :], query, NT, preferred_element_type=f32
            )

    def finish(index, score_ref, weight_ref):
        at = lax.broadcasted_iota(i32, (1, BLOCK), 1) + BLOCK
        low = at - back_ref[:, block(index)]
        high = jnp.minimum(at + ahead_ref[:, block(index)], live - (index - 1) * BLOCK - 1)
        total = jnp.zeros((1, BLOCK), f32)
        for k in range(3):
            slot = lax.broadcasted_iota(i32, (BLOCK, BLOCK), 0) + k * BLOCK
            keep = (slot >= low, ((slot >= low) & (slot <= high)) | (slot == at), slot <= high)[k]
            span = slice(k * BLOCK, (k + 1) * BLOCK)
            weight = jnp.where(keep, jnp.exp2(score_ref[span, :] * SCALE - SCALE), 0.0)
            total = total + jnp.sum(weight, axis=0, keepdims=True)
            weight_ref[span, :] = weight.astype(bf16)
        keys_t = unit_t_ref[:, pl.ds(pl.multiple_of((index - 1) * BLOCK, BLOCK), 3 * BLOCK)]
        mixed = jnp.dot(keys_t, weight_ref[...], preferred_element_type=f32)
        out_ref[:, block(index - 1)] = (mixed * (1.0 / total)).astype(bf16)

    def early(index, _):
        prepare(index)
        return 0

    lax.fori_loop(0, 4, early, 0)
    score(1, score_a)

    def step(pair, _):
        index = 2 * pair + 1
        score(index + 1, score_b)
        finish(index, score_a, weight_a)
        prepare(jnp.minimum(index + 3, NBLK - 1))
        score(jnp.minimum(index + 2, NBLK - 2), score_a)
        finish(index + 1, score_b, weight_b)
        prepare(jnp.minimum(index + 4, NBLK - 1))
        return 0

    lax.fori_loop(0, (NBLK - 2) // 2, step, 0)


def edges_kernel(live_ref, back_ref, ahead_ref, spectra_ref, below_ref, above_ref, out_ref):
    live = live_ref[0]

    def count(ref):
        digits = ref[BLOCK : BLOCK + 8, :BLOCK].astype(f32)
        return (digits[0:1] * 64.0 + digits[1:2]).astype(i32)

    def unit(block):
        return unit_rows(spectra_ref[block * BLOCK : (block + 1) * BLOCK, :])

    keys = [unit_rows(below_ref[:BLOCK, :]), unit(0), unit(1)]
    out_ref[:, :BLOCK] = attend(
        keys[1], back_ref[:, :BLOCK], ahead_ref[:, :BLOCK], live + BLOCK, keys,
        [transposed(k) for k in keys], count(below_ref) - (ROWS - BLOCK), None,
    )
    keys = [unit(NBLK - 2), unit(NBLK - 1), unit_rows(above_ref[:BLOCK, :])]
    out_ref[:, BLOCK:] = attend(
        keys[1], back_ref[:, ROWS - BLOCK :], ahead_ref[:, ROWS - BLOCK :],
        live - (ROWS - 2 * BLOCK), keys, [transposed(k) for k in keys],
        None, count(above_ref) + 2 * BLOCK,
    )


INNER = ROWS - 2 * BLOCK
CHUNK = INNER // 4


def added(first, live, ids_ref, rows, start):
    width = rows.shape[1]
    slot = lax.broadcasted_iota(i32, (1, width), 1) + start
    wanted = jnp.where(slot < live, ids_ref[:, start : start + width] - first, FAR)
    hot = lax.broadcasted_iota(i32, (CL_DEV, width), 0) == wanted
    hot = jnp.where(hot, 1.0, 0.0).astype(bf16)
    return lax.dot_general(hot, rows, NT, preferred_element_type=f32)


def sums_kernel(turns, away, halves, rep_count, live_ref, ids_ref, inner_ref, edge_ref, *outs):
    rep = lax.axis_index("rep")
    band = lax.axis_index("mz")
    per_range = CL_DEV * rep_count
    if away:
        band = band + jnp.where(rep == 0, -1, 1)

    def work():
        live = live_ref[0]
        for turn, out_ref in zip(turns, outs):
            owner = lax.rem(rep + turn, rep_count)
            first = band * per_range + owner * CL_DEV

            acc = added(first, live, ids_ref, edge_ref[:, :BLOCK], 0)
            acc = acc + added(first, live, ids_ref, edge_ref[:, BLOCK:], ROWS - BLOCK)
            for start in range(0, INNER, CHUNK):
                acc = acc + added(first, live, ids_ref, inner_ref[:, start : start + CHUNK], start + BLOCK)
            acc = acc.astype(out_ref.dtype)
            if halves:
                outs[0][...] = acc[: CL_DEV // 2]
                outs[1][...] = acc[CL_DEV // 2 :]
            else:
                out_ref[...] = acc

    if away:
        pl.when((rep == 0) | (rep == rep_count - 1))(work)
    else:
        work()


def join_kernel(own_up, own_down, low_half, high_half, moved_1, moved_2, next_up, next_down):
    rep, last = lax.axis_index("rep"), lax.axis_size("rep") - 1
    half = CL_DEV // 2
    far = moved_2[...].astype(f32)
    above = own_up[...] + moved_1[...].astype(f32) + jnp.where(rep == 1, far, 0.0)
    below = own_down[...] + jnp.where(rep == last - 1, far, 0.0)
    next_up[:half, :] = (above[:half] + low_half[...].astype(f32)).astype(bf16)
    next_up[half:, :] = above[half:].astype(bf16)
    next_down[:half, :] = below[:half].astype(bf16)
    next_down[half:, :] = (below[half:] + high_half[...].astype(f32)).astype(bf16)


def finish_kernel(own_ref, *rest):
    out_ref = rest[-1]
    owned = own_ref[...]
    for ref in rest[:-1]:
        owned = owned + ref[...].astype(f32)
    mean = jnp.sum(owned * owned, axis=1, keepdims=True) * (1.0 / DIM)
    out_ref[...] = owned / jnp.sqrt(mean + 1e-06)


VMEM = pl.BlockSpec(memory_space=pltpu.VMEM)
SMEM = pl.BlockSpec(memory_space=pltpu.SMEM)
FARREF = pl.BlockSpec(memory_space=pltpu.HBM)
MIB = 1024 * 1024


def call(kernel, inputs, out_shape, flops, scratch=(), far=(), limit=16):
    one = not isinstance(out_shape, (list, tuple))
    in_specs = [
        FARREF if n in far else SMEM if x.dtype == i32 and x.size < 64 else VMEM for n, x in enumerate(inputs)
    ]
    moved = sum(x.size * x.dtype.itemsize for x in inputs)
    return pl.pallas_call(
        kernel,
        out_shape=out_shape,
        in_specs=in_specs,
        out_specs=VMEM if one else [VMEM] * len(out_shape),
        scratch_shapes=list(scratch),
        cost_estimate=pl.CostEstimate(flops=flops, bytes_accessed=moved, transcendentals=0),
        compiler_params=pltpu.CompilerParams(vmem_limit_bytes=limit * MIB),
    )(*inputs)


def shape(rows, columns, dtype):
    return jax.ShapeDtypeStruct((rows, columns), dtype)


def shards(spectra, reach_back, reach_ahead, live, cluster_ids):
    bands, reps = lax.axis_size("mz"), lax.axis_size("rep")
    every = bands * reps
    both = ("mz", "rep")

    def sum_blocks(turns, away, dtype, halves=False):
        outs = [shape(CL_DEV // 2, DIM, dtype)] * 2 if halves else [shape(CL_DEV, DIM, dtype)] * len(turns)
        return call(
            functools.partial(sums_kernel, turns, away, halves, reps),
            [live, ids, inner, edge], outs,
            2 * CL_DEV * ROWS * DIM * len(turns),
        )

    back, ahead, ids = (x.reshape(1, ROWS) for x in (reach_back, reach_ahead, cluster_ids))
    low_rows, high_rows = call(
        pack_kernel, [live, spectra[:BLOCK], spectra[ROWS - BLOCK :]],
        [shape(HALO, DIM, bf16)] * 2, 1 << 33, limit=2,
    )
    from_below = lax.ppermute(high_rows, both, [(i, i + 1) for i in range(every - 1)])
    from_above = lax.ppermute(low_rows, both, [(i + 1, i) for i in range(every - 1)])
    per_block = 4 * BLOCK * 3 * BLOCK * DIM
    inner = call(
        interior_kernel, [live, back, ahead, spectra], shape(DIM, INNER, bf16), per_block * (NBLK - 2),
        [
            pltpu.VMEM((ROWS, DIM), bf16), pltpu.VMEM((DIM, ROWS), bf16),
            pltpu.VMEM((3 * BLOCK, BLOCK), f32), pltpu.VMEM((3 * BLOCK, BLOCK), f32),
            pltpu.VMEM((3 * BLOCK, BLOCK), bf16), pltpu.VMEM((3 * BLOCK, BLOCK), bf16),
        ],
        limit=32,
    )
    edge = call(
        edges_kernel, [live, back, ahead, spectra, from_below, from_above],
        shape(DIM, 2 * BLOCK, bf16), 2 * per_block,
    )

    def away_pairs(inwards):
        pairs = [(d * reps, (d - 1) * reps + inwards % reps) for d in range(1, bands)]
        return pairs + [
            (d * reps + reps - 1, (d + 1) * reps + (reps - 1 - inwards) % reps) for d in range(bands - 1)
        ]

    last = reps - 1
    up = [(i, (i + 1) % reps) for i in range(reps)]
    down = [(b, a) for a, b in up]
    low_half, high_half = sum_blocks((2,), False, bf16, halves=True)
    low_half = lax.ppermute(low_half, "rep", up)
    high_half = lax.ppermute(high_half, "rep", down)
    (block,) = sum_blocks((2,), True, bf16)
    moved_2 = lax.ppermute(block, both, away_pairs(1))
    (block,) = sum_blocks((1,), True, bf16)
    moved_1 = lax.ppermute(block, both, away_pairs(0))
    own_1, own_3 = sum_blocks((1, 3), False, f32)
    next_up, next_down = call(
        join_kernel, [own_1, own_3, low_half, high_half, moved_1, moved_2],
        [shape(CL_DEV, DIM, bf16)] * 2, 1 << 20,
    )
    got_up = lax.ppermute(next_up, "rep", up)
    got_down = lax.ppermute(next_down, "rep", down)
    (block,) = sum_blocks((3,), True, bf16)
    pairs = [(d * reps, (d - 1) * reps + last) for d in range(1, bands)]
    pairs += [(d * reps + last, (d + 1) * reps + last - 1) for d in range(bands - 1)]
    moved_3 = lax.ppermute(block, both, pairs)
    (block,) = sum_blocks((0,), True, bf16)
    moved_0 = lax.ppermute(block, both, away_pairs(0))
    (own_0,) = sum_blocks((0,), False, f32)
    return call(finish_kernel, [own_0, got_up, got_down, moved_3, moved_0], shape(CL_DEV, DIM, f32), 1 << 20)


def solution(mesh):
    rows = P(("mz", "rep"))

    return jax.shard_map(
        shards,
        mesh=mesh,
        in_specs=(P(("mz", "rep"), None), rows, rows, rows, rows),
        out_specs=P(("mz", "rep"), None),
        check_vma=False,
    )
```

```python
import functools

import jax
import jax.numpy as jnp
from jax import lax
from jax.experimental import pallas as pl
from jax.experimental.pallas import tpu as pltpu
from jax.sharding import PartitionSpec as P


DIM = 512
BLOCK = 256
CL_DEV = 512
ROWS = 4096
NBLK = ROWS // BLOCK
HALO = BLOCK + 16
FAR = -(1 << 24)
SCALE = 3.0 * 1.4426950408889634
f32, bf16, i32 = jnp.float32, jnp.bfloat16, jnp.int32
NT = (((1,), (1,)), ((), ()))


def unit_rows(block):
    values = block.astype(f32)
    square = jnp.sum(values * values, axis=1, keepdims=True)
    return (values * lax.rsqrt(square + 1e-06)).astype(bf16)


def transposed(unit):
    return jnp.transpose(unit)


def attend(query, back, ahead, cap, keys, keys_t, low_cap, high_cap):
    at = lax.broadcasted_iota(i32, (1, BLOCK), 1) + BLOCK
    low = at - back
    high = at + ahead
    own = jnp.minimum(high, cap - 1)
    total = None
    mixed = None
    for k in range(3):
        scores = lax.dot_general(keys[k], query, NT, preferred_element_type=f32)
        slot = lax.broadcasted_iota(i32, (BLOCK, BLOCK), 0) + k * BLOCK
        if k == 0:
            keep = slot >= low
            if low_cap is not None:
                keep = keep & (slot < low_cap)
        elif k == 1:
            keep = ((slot >= low) & (slot <= own)) | (slot == at)
        elif high_cap is None:
            keep = slot <= own
        else:
            keep = slot <= jnp.minimum(high, high_cap - 1)
        weight = jnp.where(keep, jnp.exp2(scores * SCALE - SCALE), 0.0)
        part = jnp.sum(weight, axis=0, keepdims=True)
        term = jnp.dot(keys_t[k], weight.astype(bf16), preferred_element_type=f32)
        total = part if total is None else total + part
        mixed = term if mixed is None else mixed + term
    return (mixed * (1.0 / total)).astype(bf16)


def pack_kernel(live_ref, first_ref, last_ref, low_ref, high_ref):
    live = live_ref[0]
    row = lax.broadcasted_iota(i32, (HALO - BLOCK, DIM), 0)
    digits = jnp.where(row == 0, live >> 6, live & 63).astype(f32).astype(bf16)
    for source, ref in ((first_ref, low_ref), (last_ref, high_ref)):
        ref[:BLOCK, :] = source[...]
        ref[BLOCK:, :] = digits


def interior_kernel(
    live_ref, back_ref, ahead_ref, rows_ref, out_ref,
    unit_ref, unit_t_ref, score_a, score_b, weight_a, weight_b,
):
    live = live_ref[0]

    def block(index):
        return pl.ds(pl.multiple_of(index * BLOCK, BLOCK), BLOCK)

    def prepare(index):
        unit = unit_rows(rows_ref[block(index), :])
        unit_ref[block(index), :] = unit
        unit_t_ref[:, block(index)] = transposed(unit)

    def score(index, score_ref):
        query = unit_ref[block(index), :]
        for k in range(3):
            score_ref[k * BLOCK : (k + 1) * BLOCK, :] = lax.dot_general(
                unit_ref[block(index + k - 1), :], query, NT, preferred_element_type=f32
            )

    def finish(index, score_ref, weight_ref):
        at = lax.broadcasted_iota(i32, (1, BLOCK), 1) + BLOCK
        low = at - back_ref[:, block(index)]
        high = jnp.minimum(at + ahead_ref[:, block(index)], live - (index - 1) * BLOCK - 1)
        total = jnp.zeros((1, BLOCK), f32)
        for k in range(3):
            slot = lax.broadcasted_iota(i32, (BLOCK, BLOCK), 0) + k * BLOCK
            keep = (slot >= low, ((slot >= low) & (slot <= high)) | (slot == at), slot <= high)[k]
            span = slice(k * BLOCK, (k + 1) * BLOCK)
            weight = jnp.where(keep, jnp.exp2(score_ref[span, :] * SCALE - SCALE), 0.0)
            total = total + jnp.sum(weight, axis=0, keepdims=True)
            weight_ref[span, :] = weight.astype(bf16)
        keys_t = unit_t_ref[:, pl.ds(pl.multiple_of((index - 1) * BLOCK, BLOCK), 3 * BLOCK)]
        mixed = jnp.dot(keys_t, weight_ref[...], preferred_element_type=f32)
        out_ref[:, block(index - 1)] = (mixed * (1.0 / total)).astype(bf16)

    def early(index, _):
        prepare(index)
        return 0

    lax.fori_loop(0, 4, early, 0)
    score(1, score_a)

    def step(pair, _):
        index = 2 * pair + 1
        score(index + 1, score_b)
        finish(index, score_a, weight_a)
        prepare(jnp.minimum(index + 3, NBLK - 1))
        score(jnp.minimum(index + 2, NBLK - 2), score_a)
        finish(index + 1, score_b, weight_b)
        prepare(jnp.minimum(index + 4, NBLK - 1))
        return 0

    lax.fori_loop(0, (NBLK - 2) // 2, step, 0)


def edges_kernel(live_ref, back_ref, ahead_ref, spectra_ref, below_ref, above_ref, out_ref):
    live = live_ref[0]

    def count(ref):
        digits = ref[BLOCK : BLOCK + 8, :BLOCK].astype(f32)
        return (digits[0:1] * 64.0 + digits[1:2]).astype(i32)

    def unit(block):
        return unit_rows(spectra_ref[block * BLOCK : (block + 1) * BLOCK, :])

    keys = [unit_rows(below_ref[:BLOCK, :]), unit(0), unit(1)]
    out_ref[:, :BLOCK] = attend(
        keys[1], back_ref[:, :BLOCK], ahead_ref[:, :BLOCK], live + BLOCK, keys,
        [transposed(k) for k in keys], count(below_ref) - (ROWS - BLOCK), None,
    )
    keys = [unit(NBLK - 2), unit(NBLK - 1), unit_rows(above_ref[:BLOCK, :])]
    out_ref[:, BLOCK:] = attend(
        keys[1], back_ref[:, ROWS - BLOCK :], ahead_ref[:, ROWS - BLOCK :],
        live - (ROWS - 2 * BLOCK), keys, [transposed(k) for k in keys],
        None, count(above_ref) + 2 * BLOCK,
    )


INNER = ROWS - 2 * BLOCK
CHUNK = INNER // 4


def added(first, live, ids_ref, rows, start):
    width = rows.shape[1]
    slot = lax.broadcasted_iota(i32, (1, width), 1) + start
    wanted = jnp.where(slot < live, ids_ref[:, start : start + width] - first, FAR)
    hot = lax.broadcasted_iota(i32, (CL_DEV, width), 0) == wanted
    hot = jnp.where(hot, 1.0, 0.0).astype(bf16)
    return lax.dot_general(hot, rows, NT, preferred_element_type=f32)


def sums_kernel(turns, away, rep_count, live_ref, ids_ref, inner_ref, edge_ref, *outs):
    rep = lax.axis_index("rep")
    band = lax.axis_index("mz")
    per_range = CL_DEV * rep_count
    if away:
        band = band + jnp.where(rep == 0, -1, 1)

    def work():
        live = live_ref[0]
        for turn, out_ref in zip(turns, outs):
            owner = lax.rem(rep + turn, rep_count)
            first = band * per_range + owner * CL_DEV

            acc = added(first, live, ids_ref, edge_ref[:, :BLOCK], 0)
            acc = acc + added(first, live, ids_ref, edge_ref[:, BLOCK:], ROWS - BLOCK)
            for start in range(0, INNER, CHUNK):
                acc = acc + added(first, live, ids_ref, inner_ref[:, start : start + CHUNK], start + BLOCK)
            out_ref[...] = acc.astype(out_ref.dtype)

    if away:
        pl.when((rep == 0) | (rep == rep_count - 1))(work)
    else:
        work()


def far_kernel(own_ref, moved_ref, low_ref, high_ref):
    total = (own_ref[...] + moved_ref[...].astype(f32)).astype(bf16)
    low_ref[...] = total[: CL_DEV // 2]
    high_ref[...] = total[CL_DEV // 2 :]


def join_kernel(own_up, own_down, low_half, high_half, moved_1, moved_3, next_up, next_down):
    half = CL_DEV // 2
    above = own_up[...] + moved_1[...].astype(f32)
    below = own_down[...] + moved_3[...].astype(f32)
    next_up[:half, :] = (above[:half] + low_half[...].astype(f32)).astype(bf16)
    next_up[half:, :] = above[half:].astype(bf16)
    next_down[:half, :] = below[:half].astype(bf16)
    next_down[half:, :] = (below[half:] + high_half[...].astype(f32)).astype(bf16)


def finish_kernel(own_ref, *rest):
    out_ref = rest[-1]
    owned = own_ref[...]
    for ref in rest[:-1]:
        owned = owned + ref[...].astype(f32)
    mean = jnp.sum(owned * owned, axis=1, keepdims=True) * (1.0 / DIM)
    out_ref[...] = owned / jnp.sqrt(mean + 1e-06)


VMEM = pl.BlockSpec(memory_space=pltpu.VMEM)
SMEM = pl.BlockSpec(memory_space=pltpu.SMEM)
FARREF = pl.BlockSpec(memory_space=pltpu.HBM)
MIB = 1024 * 1024


def call(kernel, inputs, out_shape, flops, scratch=(), far=(), limit=16):
    one = not isinstance(out_shape, (list, tuple))
    in_specs = [
        FARREF if n in far else SMEM if x.dtype == i32 and x.size < 64 else VMEM for n, x in enumerate(inputs)
    ]
    moved = sum(x.size * x.dtype.itemsize for x in inputs)
    return pl.pallas_call(
        kernel,
        out_shape=out_shape,
        in_specs=in_specs,
        out_specs=VMEM if one else [VMEM] * len(out_shape),
        scratch_shapes=list(scratch),
        cost_estimate=pl.CostEstimate(flops=flops, bytes_accessed=moved, transcendentals=0),
        compiler_params=pltpu.CompilerParams(vmem_limit_bytes=limit * MIB),
    )(*inputs)


def shape(rows, columns, dtype):
    return jax.ShapeDtypeStruct((rows, columns), dtype)


def shards(spectra, reach_back, reach_ahead, live, cluster_ids):
    bands, reps = lax.axis_size("mz"), lax.axis_size("rep")
    every = bands * reps
    both = ("mz", "rep")

    def sum_blocks(turns, away, dtype):
        outs = [shape(CL_DEV, DIM, dtype)] * len(turns)
        return call(
            functools.partial(sums_kernel, turns, away, reps),
            [live, ids, inner, edge], outs,
            2 * CL_DEV * ROWS * DIM * len(turns),
        )

    back, ahead, ids = (x.reshape(1, ROWS) for x in (reach_back, reach_ahead, cluster_ids))
    low_rows, high_rows = call(
        pack_kernel, [live, spectra[:BLOCK], spectra[ROWS - BLOCK :]],
        [shape(HALO, DIM, bf16)] * 2, 1 << 33, limit=2,
    )
    from_below = lax.ppermute(high_rows, both, [(i, i + 1) for i in range(every - 1)])
    from_above = lax.ppermute(low_rows, both, [(i + 1, i) for i in range(every - 1)])
    per_block = 4 * BLOCK * 3 * BLOCK * DIM
    inner = call(
        interior_kernel, [live, back, ahead, spectra], shape(DIM, INNER, bf16), per_block * (NBLK - 2),
        [
            pltpu.VMEM((ROWS, DIM), bf16), pltpu.VMEM((DIM, ROWS), bf16),
            pltpu.VMEM((3 * BLOCK, BLOCK), f32), pltpu.VMEM((3 * BLOCK, BLOCK), f32),
            pltpu.VMEM((3 * BLOCK, BLOCK), bf16), pltpu.VMEM((3 * BLOCK, BLOCK), bf16),
        ],
        limit=32,
    )
    edge = call(
        edges_kernel, [live, back, ahead, spectra, from_below, from_above],
        shape(DIM, 2 * BLOCK, bf16), 2 * per_block,
    )

    last = reps - 1
    away_pairs = [(d * reps, (d - 1) * reps) for d in range(1, bands)]
    away_pairs += [(d * reps + last, (d + 1) * reps + last) for d in range(bands - 1)]
    up = [(i, (i + 1) % reps) for i in range(reps)]
    down = [(b, a) for a, b in up]
    arrived = {}
    own = {}

    def send_away(turn):
        (block,) = sum_blocks((turn,), True, bf16)
        arrived[turn] = lax.ppermute(block, both, away_pairs)

    send_away(2)
    (own[2],) = sum_blocks((2,), False, f32)
    send_away(1)
    half = shape(CL_DEV // 2, DIM, bf16)
    low_half, high_half = call(far_kernel, [own[2], arrived[2]], [half] * 2, 1 << 20)
    low_half = lax.ppermute(low_half, "rep", up)
    high_half = lax.ppermute(high_half, "rep", down)
    send_away(3)
    own[1], own[3] = sum_blocks((1, 3), False, f32)
    next_up, next_down = call(
        join_kernel, [own[1], own[3], low_half, high_half, arrived[1], arrived[3]],
        [shape(CL_DEV, DIM, bf16)] * 2, 1 << 20,
    )
    got_up = lax.ppermute(next_up, "rep", up)
    got_down = lax.ppermute(next_down, "rep", down)
    send_away(0)
    (own[0],) = sum_blocks((0,), False, f32)
    return call(finish_kernel, [own[0], got_up, got_down, arrived[0]], shape(CL_DEV, DIM, f32), 1 << 20)


def solution(mesh):
    rows = P(("mz", "rep"))

    return jax.shard_map(
        shards,
        mesh=mesh,
        in_specs=(P(("mz", "rep"), None), rows, rows, rows, rows),
        out_specs=P(("mz", "rep"), None),
        check_vma=False,
    )
```

```python
import functools

import jax
import jax.numpy as jnp
from jax import lax
from jax.experimental import pallas as pl
from jax.experimental.pallas import tpu as pltpu
from jax.sharding import PartitionSpec as P


DIM = 512
BLOCK = 256
CL_DEV = 512
ROWS = 4096
NBLK = ROWS // BLOCK
HALO = BLOCK + 16
FAR = -(1 << 24)
SCALE = 3.0 * 1.4426950408889634
f32, bf16, i32 = jnp.float32, jnp.bfloat16, jnp.int32
NT = (((1,), (1,)), ((), ()))


def unit_rows(block):
    values = block.astype(f32)
    square = jnp.sum(values * values, axis=1, keepdims=True)
    return (values * lax.rsqrt(square + 1e-06)).astype(bf16)


def transposed(unit):
    return jnp.transpose(unit)


def attend(query, back, ahead, cap, keys, keys_t, low_cap, high_cap):
    at = lax.broadcasted_iota(i32, (1, BLOCK), 1) + BLOCK
    low = at - back
    high = at + ahead
    own = jnp.minimum(high, cap - 1)
    total = None
    mixed = None
    for k in range(3):
        scores = lax.dot_general(keys[k], query, NT, preferred_element_type=f32)
        slot = lax.broadcasted_iota(i32, (BLOCK, BLOCK), 0) + k * BLOCK
        if k == 0:
            keep = slot >= low
            if low_cap is not None:
                keep = keep & (slot < low_cap)
        elif k == 1:
            keep = ((slot >= low) & (slot <= own)) | (slot == at)
        elif high_cap is None:
            keep = slot <= own
        else:
            keep = slot <= jnp.minimum(high, high_cap - 1)
        weight = jnp.where(keep, jnp.exp2(scores * SCALE - SCALE), 0.0)
        part = jnp.sum(weight, axis=0, keepdims=True)
        term = jnp.dot(keys_t[k], weight.astype(bf16), preferred_element_type=f32)
        total = part if total is None else total + part
        mixed = term if mixed is None else mixed + term
    return (mixed * (1.0 / total)).astype(bf16)


def pack_kernel(live_ref, first_ref, last_ref, low_ref, high_ref):
    live = live_ref[0]
    row = lax.broadcasted_iota(i32, (HALO - BLOCK, DIM), 0)
    digits = jnp.where(row == 0, live >> 6, live & 63).astype(f32).astype(bf16)
    for source, ref in ((first_ref, low_ref), (last_ref, high_ref)):
        ref[:BLOCK, :] = source[...]
        ref[BLOCK:, :] = digits


def interior_kernel(
    live_ref, back_ref, ahead_ref, rows_ref, out_ref,
    unit_ref, unit_t_ref, score_a, score_b, weight_a, weight_b,
):
    live = live_ref[0]

    def block(index):
        return pl.ds(pl.multiple_of(index * BLOCK, BLOCK), BLOCK)

    def prepare(index):
        unit = unit_rows(rows_ref[block(index), :])
        unit_ref[block(index), :] = unit
        unit_t_ref[:, block(index)] = transposed(unit)

    def score(index, score_ref):
        query = unit_ref[block(index), :]
        for k in range(3):
            score_ref[k * BLOCK : (k + 1) * BLOCK, :] = lax.dot_general(
                unit_ref[block(index + k - 1), :], query, NT, preferred_element_type=f32
            )

    def finish(index, score_ref, weight_ref):
        at = lax.broadcasted_iota(i32, (1, BLOCK), 1) + BLOCK
        low = at - back_ref[:, block(index)]
        high = jnp.minimum(at + ahead_ref[:, block(index)], live - (index - 1) * BLOCK - 1)
        total = jnp.zeros((1, BLOCK), f32)
        for k in range(3):
            slot = lax.broadcasted_iota(i32, (BLOCK, BLOCK), 0) + k * BLOCK
            keep = (slot >= low, ((slot >= low) & (slot <= high)) | (slot == at), slot <= high)[k]
            span = slice(k * BLOCK, (k + 1) * BLOCK)
            weight = jnp.where(keep, jnp.exp2(score_ref[span, :] * SCALE - SCALE), 0.0)
            total = total + jnp.sum(weight, axis=0, keepdims=True)
            weight_ref[span, :] = weight.astype(bf16)
        keys_t = unit_t_ref[:, pl.ds(pl.multiple_of((index - 1) * BLOCK, BLOCK), 3 * BLOCK)]
        mixed = jnp.dot(keys_t, weight_ref[...], preferred_element_type=f32)
        out_ref[:, block(index - 1)] = (mixed * (1.0 / total)).astype(bf16)

    def early(index, _):
        prepare(index)
        return 0

    lax.fori_loop(0, 4, early, 0)
    score(1, score_a)

    def step(pair, _):
        index = 2 * pair + 1
        score(index + 1, score_b)
        finish(index, score_a, weight_a)
        prepare(jnp.minimum(index + 3, NBLK - 1))
        score(jnp.minimum(index + 2, NBLK - 2), score_a)
        finish(index + 1, score_b, weight_b)
        prepare(jnp.minimum(index + 4, NBLK - 1))
        return 0

    lax.fori_loop(0, (NBLK - 2) // 2, step, 0)


def edges_kernel(live_ref, back_ref, ahead_ref, spectra_ref, below_ref, above_ref, out_ref):
    live = live_ref[0]

    def count(ref):
        digits = ref[BLOCK : BLOCK + 8, :BLOCK].astype(f32)
        return (digits[0:1] * 64.0 + digits[1:2]).astype(i32)

    def unit(block):
        return unit_rows(spectra_ref[block * BLOCK : (block + 1) * BLOCK, :])

    keys = [unit_rows(below_ref[:BLOCK, :]), unit(0), unit(1)]
    out_ref[:, :BLOCK] = attend(
        keys[1], back_ref[:, :BLOCK], ahead_ref[:, :BLOCK], live + BLOCK, keys,
        [transposed(k) for k in keys], count(below_ref) - (ROWS - BLOCK), None,
    )
    keys = [unit(NBLK - 2), unit(NBLK - 1), unit_rows(above_ref[:BLOCK, :])]
    out_ref[:, BLOCK:] = attend(
        keys[1], back_ref[:, ROWS - BLOCK :], ahead_ref[:, ROWS - BLOCK :],
        live - (ROWS - 2 * BLOCK), keys, [transposed(k) for k in keys],
        None, count(above_ref) + 2 * BLOCK,
    )


INNER = ROWS - 2 * BLOCK
CHUNK = 512


def partners(rep, parity, rep_count):
    across = rep_count - 1 - rep
    beside = rep + 1 - 2 * (rep & 1)
    if isinstance(rep, int):
        return (beside, across) if parity else (across, beside)
    odd = parity == 1
    return jnp.where(odd, beside, across), jnp.where(odd, across, beside)


def sums_kernel(first_step, away, rep_count, live_ref, ids_ref, inner_ref, edge_ref, out_ref):
    rep = lax.axis_index("rep")
    band = lax.axis_index("mz")
    if away:
        band = band + jnp.where(rep == 0, -1, 1)
    one, two = partners(rep, band & 1, rep_count)
    owners = (partners(one, band & 1, rep_count)[1], one) if first_step else (two, rep)
    firsts = [band * (CL_DEV * rep_count) + owner * CL_DEV for owner in owners]

    def work():
        live = live_ref[0]
        lane = lax.broadcasted_iota(i32, (1, BLOCK), 1)

        def added(pieces, rows):
            wanted = jnp.concatenate(
                [
                    jnp.where(lane + start < live, ids_ref[:, start : start + BLOCK], FAR)
                    for start in pieces
                ],
                axis=1,
            )
            cluster = lax.broadcasted_iota(i32, (CL_DEV, CHUNK), 0)
            hot = jnp.concatenate(
                [jnp.where(cluster == wanted - first, 1.0, 0.0).astype(bf16) for first in firsts], axis=0
            )
            return lax.dot_general(hot, rows, NT, preferred_element_type=f32)

        acc = added((0, ROWS - BLOCK), edge_ref[...])
        for start in range(0, INNER, CHUNK):
            pieces = range(start + BLOCK, start + BLOCK + CHUNK, BLOCK)
            acc = acc + added(pieces, inner_ref[:, start : start + CHUNK])
        out_ref[...] = acc.astype(out_ref.dtype)

    if away:
        pl.when((rep == 0) | (rep == rep_count - 1))(work)
    else:
        work()


def far_kernel(own_ref, moved_ref, out_ref):
    out_ref[...] = (own_ref[...] + moved_ref[...].astype(f32)).astype(bf16)


def join_kernel(own_ref, moved_ref, got_ref, next_ref, mine_ref):
    for half, ref in ((slice(0, CL_DEV), next_ref), (slice(CL_DEV, 2 * CL_DEV), mine_ref)):
        total = own_ref[half, :] + moved_ref[half, :].astype(f32) + got_ref[half, :].astype(f32)
        ref[...] = total.astype(ref.dtype)


def finish_kernel(mine_ref, got_ref, out_ref):
    owned = mine_ref[...] + got_ref[...].astype(f32)
    mean = jnp.sum(owned * owned, axis=1, keepdims=True) * (1.0 / DIM)
    out_ref[...] = owned / jnp.sqrt(mean + 1e-06)


VMEM = pl.BlockSpec(memory_space=pltpu.VMEM)
SMEM = pl.BlockSpec(memory_space=pltpu.SMEM)
FARREF = pl.BlockSpec(memory_space=pltpu.HBM)
MIB = 1024 * 1024


def call(kernel, inputs, out_shape, flops, scratch=(), far=(), limit=16):
    one = not isinstance(out_shape, (list, tuple))
    in_specs = [
        FARREF if n in far else SMEM if x.dtype == i32 and x.size < 64 else VMEM for n, x in enumerate(inputs)
    ]
    moved = sum(x.size * x.dtype.itemsize for x in inputs)
    return pl.pallas_call(
        kernel,
        out_shape=out_shape,
        in_specs=in_specs,
        out_specs=VMEM if one else [VMEM] * len(out_shape),
        scratch_shapes=list(scratch),
        cost_estimate=pl.CostEstimate(flops=flops, bytes_accessed=moved, transcendentals=0),
        compiler_params=pltpu.CompilerParams(vmem_limit_bytes=limit * MIB),
    )(*inputs)


def shape(rows, columns, dtype):
    return jax.ShapeDtypeStruct((rows, columns), dtype)


def shards(spectra, reach_back, reach_ahead, live, cluster_ids):
    bands, reps = lax.axis_size("mz"), lax.axis_size("rep")
    every = bands * reps
    both = ("mz", "rep")

    def sum_pair(first_step, away, dtype):
        return call(
            functools.partial(sums_kernel, first_step, away, reps),
            [live, ids, inner, edge], shape(2 * CL_DEV, DIM, dtype), 4 * CL_DEV * ROWS * DIM, limit=20,
        )

    back, ahead, ids = (x.reshape(1, ROWS) for x in (reach_back, reach_ahead, cluster_ids))
    low_rows, high_rows = call(
        pack_kernel, [live, spectra[:BLOCK], spectra[ROWS - BLOCK :]],
        [shape(HALO, DIM, bf16)] * 2, 1 << 33, limit=2,
    )
    from_below = lax.ppermute(high_rows, both, [(i, i + 1) for i in range(every - 1)])
    from_above = lax.ppermute(low_rows, both, [(i + 1, i) for i in range(every - 1)])
    per_block = 4 * BLOCK * 3 * BLOCK * DIM
    inner = call(
        interior_kernel, [live, back, ahead, spectra], shape(DIM, INNER, bf16), per_block * (NBLK - 2),
        [
            pltpu.VMEM((ROWS, DIM), bf16), pltpu.VMEM((DIM, ROWS), bf16),
            pltpu.VMEM((3 * BLOCK, BLOCK), f32), pltpu.VMEM((3 * BLOCK, BLOCK), f32),
            pltpu.VMEM((3 * BLOCK, BLOCK), bf16), pltpu.VMEM((3 * BLOCK, BLOCK), bf16),
        ],
        limit=32,
    )
    edge = call(
        edges_kernel, [live, back, ahead, spectra, from_below, from_above],
        shape(DIM, 2 * BLOCK, bf16), 2 * per_block,
    )

    last = reps - 1
    away_pairs = [(d * reps, (d - 1) * reps) for d in range(1, bands)]
    away_pairs += [(d * reps + last, (d + 1) * reps + last) for d in range(bands - 1)]
    swaps = [
        [(d * reps + r, d * reps + partners(r, d & 1, reps)[step]) for d in range(bands) for r in range(reps)]
        for step in range(2)
    ]
    x_far = lax.ppermute(sum_pair(True, True, bf16), both, away_pairs)
    x_near = lax.ppermute(sum_pair(False, True, bf16), both, away_pairs)
    own_far = sum_pair(True, False, f32)
    far = call(far_kernel, [own_far, x_far], shape(2 * CL_DEV, DIM, bf16), 1 << 20)
    got_first = lax.ppermute(far, both, swaps[0])
    own_near = sum_pair(False, False, f32)
    after_first, mine = call(
        join_kernel, [own_near, x_near, got_first],
        [shape(CL_DEV, DIM, bf16), shape(CL_DEV, DIM, f32)], 1 << 20,
    )
    got_second = lax.ppermute(after_first, both, swaps[1])
    return call(finish_kernel, [mine, got_second], shape(CL_DEV, DIM, f32), 1 << 20)


def solution(mesh):
    rows = P(("mz", "rep"))

    return jax.shard_map(
        shards,
        mesh=mesh,
        in_specs=(P(("mz", "rep"), None), rows, rows, rows, rows),
        out_specs=P(("mz", "rep"), None),
        check_vma=False,
    )
```

```python
import functools

import jax
import jax.numpy as jnp
from jax import lax
from jax.experimental import pallas as pl
from jax.experimental.pallas import tpu as pltpu
from jax.sharding import PartitionSpec as P


DIM = 512
BLOCK = 256
CL_DEV = 512
ROWS = 4096
NBLK = ROWS // BLOCK
HALO = BLOCK + 16
FAR = -(1 << 24)
SCALE = 3.0 * 1.4426950408889634
f32, bf16, i32 = jnp.float32, jnp.bfloat16, jnp.int32
NT = (((1,), (1,)), ((), ()))


def unit_rows(block):
    values = block.astype(f32)
    square = jnp.sum(values * values, axis=1, keepdims=True)
    return (values * lax.rsqrt(square + 1e-06)).astype(bf16)


def transposed(unit):
    return jnp.transpose(unit)


def attend(query, back, ahead, cap, keys, keys_t, low_cap, high_cap):
    at = lax.broadcasted_iota(i32, (1, BLOCK), 1) + BLOCK
    low = at - back
    high = at + ahead
    own = jnp.minimum(high, cap - 1)
    total = None
    mixed = None
    for k in range(3):
        scores = lax.dot_general(keys[k], query, NT, preferred_element_type=f32)
        slot = lax.broadcasted_iota(i32, (BLOCK, BLOCK), 0) + k * BLOCK
        if k == 0:
            keep = slot >= low
            if low_cap is not None:
                keep = keep & (slot < low_cap)
        elif k == 1:
            keep = ((slot >= low) & (slot <= own)) | (slot == at)
        elif high_cap is None:
            keep = slot <= own
        else:
            keep = slot <= jnp.minimum(high, high_cap - 1)
        weight = jnp.where(keep, jnp.exp2(scores * SCALE - SCALE), 0.0)
        part = jnp.sum(weight, axis=0, keepdims=True)
        term = jnp.dot(keys_t[k], weight.astype(bf16), preferred_element_type=f32)
        total = part if total is None else total + part
        mixed = term if mixed is None else mixed + term
    return (mixed * (1.0 / total)).astype(bf16)


def pack_kernel(live_ref, first_ref, last_ref, one_ref, two_ref):
    live = live_ref[0]
    row = lax.broadcasted_iota(i32, (HALO - BLOCK, DIM), 0)
    digits = jnp.where(row == 0, live >> 6, live & 63).astype(f32).astype(bf16)
    one_ref[BLOCK:, :] = digits
    two_ref[BLOCK:, :] = digits
    even = lax.axis_index("rep") % 2 == 0
    for is_even, one, two in ((True, last_ref, first_ref), (False, first_ref, last_ref)):

        @pl.when(even == is_even)
        def _():
            one_ref[:BLOCK, :] = one[...]
            two_ref[:BLOCK, :] = two[...]


def interior_kernel(
    live_ref, back_ref, ahead_ref, rows_ref, out_ref,
    unit_ref, unit_t_ref, score_a, score_b, weight_a, weight_b,
):
    live = live_ref[0]

    def block(index):
        return pl.ds(pl.multiple_of(index * BLOCK, BLOCK), BLOCK)

    def prepare(index):
        unit = unit_rows(rows_ref[block(index), :])
        unit_ref[block(index), :] = unit
        unit_t_ref[:, block(index)] = transposed(unit)

    def score(index, score_ref):
        query = unit_ref[block(index), :]
        for k in range(3):
            score_ref[k * BLOCK : (k + 1) * BLOCK, :] = lax.dot_general(
                unit_ref[block(index + k - 1), :], query, NT, preferred_element_type=f32
            )

    def finish(index, score_ref, weight_ref):
        at = lax.broadcasted_iota(i32, (1, BLOCK), 1) + BLOCK
        low = at - back_ref[:, block(index)]
        high = jnp.minimum(at + ahead_ref[:, block(index)], live - (index - 1) * BLOCK - 1)
        total = jnp.zeros((1, BLOCK), f32)
        for k in range(3):
            slot = lax.broadcasted_iota(i32, (BLOCK, BLOCK), 0) + k * BLOCK
            keep = (slot >= low, ((slot >= low) & (slot <= high)) | (slot == at), slot <= high)[k]
            span = slice(k * BLOCK, (k + 1) * BLOCK)
            weight = jnp.where(keep, jnp.exp2(score_ref[span, :] * SCALE - SCALE), 0.0)
            total = total + jnp.sum(weight, axis=0, keepdims=True)
            weight_ref[span, :] = weight.astype(bf16)
        keys_t = unit_t_ref[:, pl.ds(pl.multiple_of((index - 1) * BLOCK, BLOCK), 3 * BLOCK)]
        mixed = jnp.dot(keys_t, weight_ref[...], preferred_element_type=f32)
        out_ref[:, block(index - 1)] = (mixed * (1.0 / total)).astype(bf16)

    def early(index, _):
        prepare(index)
        return 0

    lax.fori_loop(0, 4, early, 0)
    score(1, score_a)

    def step(pair, _):
        index = 2 * pair + 1
        score(index + 1, score_b)
        finish(index, score_a, weight_a)
        prepare(jnp.minimum(index + 3, NBLK - 1))
        score(jnp.minimum(index + 2, NBLK - 2), score_a)
        finish(index + 1, score_b, weight_b)
        prepare(jnp.minimum(index + 4, NBLK - 1))
        return 0

    lax.fori_loop(0, (NBLK - 2) // 2, step, 0)


def edges_kernel(live_ref, back_ref, ahead_ref, spectra_ref, one_ref, two_ref, out_ref):
    live = live_ref[0]
    even = lax.axis_index("rep") % 2 == 0
    one, two = one_ref[...].astype(f32), two_ref[...].astype(f32)
    below = jnp.where(even, two, one)
    above = jnp.where(even, one, two)

    def count(rows):
        digits = rows[BLOCK : BLOCK + 8, :BLOCK]
        return (digits[0:1] * 64.0 + digits[1:2]).astype(i32)

    def unit(block):
        return unit_rows(spectra_ref[block * BLOCK : (block + 1) * BLOCK, :])

    keys = [unit_rows(below[:BLOCK]), unit(0), unit(1)]
    out_ref[:, :BLOCK] = attend(
        keys[1], back_ref[:, :BLOCK], ahead_ref[:, :BLOCK], live + BLOCK, keys,
        [transposed(k) for k in keys], count(below) - (ROWS - BLOCK), None,
    )
    keys = [unit(NBLK - 2), unit(NBLK - 1), unit_rows(above[:BLOCK])]
    out_ref[:, BLOCK:] = attend(
        keys[1], back_ref[:, ROWS - BLOCK :], ahead_ref[:, ROWS - BLOCK :],
        live - (ROWS - 2 * BLOCK), keys, [transposed(k) for k in keys],
        None, count(above) + 2 * BLOCK,
    )


INNER = ROWS - 2 * BLOCK
CHUNK = 512


def partners(rep, parity, rep_count):
    across = rep_count - 1 - rep
    beside = rep + 1 - 2 * (rep & 1)
    if isinstance(rep, int):
        return (beside, across) if parity else (across, beside)
    odd = parity == 1
    return jnp.where(odd, beside, across), jnp.where(odd, across, beside)


def sums_kernel(role, away, rep_count, live_ref, ids_ref, inner_ref, edge_ref, out_ref):
    rep = lax.axis_index("rep")
    band = lax.axis_index("mz")
    if away:
        band = band + jnp.where(rep == 0, -1, 1)
    one, two = partners(rep, band & 1, rep_count)
    owner = (rep, one, two, partners(one, band & 1, rep_count)[1])[role]
    first = band * (CL_DEV * rep_count) + owner * CL_DEV

    def work():
        live = live_ref[0]
        lane = lax.broadcasted_iota(i32, (1, BLOCK), 1)

        def added(pieces, rows):
            wanted = jnp.concatenate(
                [
                    jnp.where(lane + start < live, ids_ref[:, start : start + BLOCK], FAR)
                    for start in pieces
                ],
                axis=1,
            )
            cluster = lax.broadcasted_iota(i32, (CL_DEV, CHUNK), 0)
            hot = jnp.where(cluster == wanted - first, 1.0, 0.0).astype(bf16)
            return lax.dot_general(hot, rows, NT, preferred_element_type=f32)

        acc = added((0, ROWS - BLOCK), edge_ref[...])
        for start in range(0, INNER, CHUNK):
            pieces = range(start + BLOCK, start + BLOCK + CHUNK, BLOCK)
            acc = acc + added(pieces, inner_ref[:, start : start + CHUNK])
        out_ref[...] = acc.astype(out_ref.dtype)

    if away:
        pl.when((rep == 0) | (rep == rep_count - 1))(work)
    else:
        work()


def add_kernel(own_ref, *rest):
    total = own_ref[...]
    for ref in rest[:-1]:
        total = total + ref[...].astype(f32)
    rest[-1][...] = total.astype(bf16)


def finish_kernel(own_ref, *rest):
    out_ref = rest[-1]
    owned = own_ref[...]
    for ref in rest[:-1]:
        owned = owned + ref[...].astype(f32)
    mean = jnp.sum(owned * owned, axis=1, keepdims=True) * (1.0 / DIM)
    out_ref[...] = owned / jnp.sqrt(mean + 1e-06)


VMEM = pl.BlockSpec(memory_space=pltpu.VMEM)
SMEM = pl.BlockSpec(memory_space=pltpu.SMEM)
FARREF = pl.BlockSpec(memory_space=pltpu.HBM)
MIB = 1024 * 1024


def call(kernel, inputs, out_shape, flops, scratch=(), far=(), limit=16):
    one = not isinstance(out_shape, (list, tuple))
    in_specs = [
        FARREF if n in far else SMEM if x.dtype == i32 and x.size < 64 else VMEM for n, x in enumerate(inputs)
    ]
    moved = sum(x.size * x.dtype.itemsize for x in inputs)
    return pl.pallas_call(
        kernel,
        out_shape=out_shape,
        in_specs=in_specs,
        out_specs=VMEM if one else [VMEM] * len(out_shape),
        scratch_shapes=list(scratch),
        cost_estimate=pl.CostEstimate(flops=flops, bytes_accessed=moved, transcendentals=0),
        compiler_params=pltpu.CompilerParams(vmem_limit_bytes=limit * MIB),
    )(*inputs)


def shape(rows, columns, dtype):
    return jax.ShapeDtypeStruct((rows, columns), dtype)


def shards(spectra, reach_back, reach_ahead, live, cluster_ids):
    bands, reps = lax.axis_size("mz"), lax.axis_size("rep")
    every = bands * reps
    both = ("mz", "rep")

    def sum_block(role, away):
        return call(
            functools.partial(sums_kernel, role, away, reps), [live, ids, inner, edge],
            shape(CL_DEV, DIM, bf16 if away else f32), 2 * CL_DEV * ROWS * DIM,
        )

    back, ahead, ids = (x.reshape(1, ROWS) for x in (reach_back, reach_ahead, cluster_ids))
    blocks = call(
        pack_kernel, [live, spectra[:BLOCK], spectra[ROWS - BLOCK :]],
        [shape(HALO, DIM, bf16)] * 2, 1 << 33, limit=2,
    )
    pairs = [(i, i + 1) for i in range(every - 1)]
    halos = [
        lax.ppermute(block, both, sorted(pair[::way] for pair in pairs[turn::2] for way in (1, -1)))
        for turn, block in enumerate(blocks)
    ]
    per_block = 4 * BLOCK * 3 * BLOCK * DIM
    inner = call(
        interior_kernel, [live, back, ahead, spectra], shape(DIM, INNER, bf16), per_block * (NBLK - 2),
        [
            pltpu.VMEM((ROWS, DIM), bf16), pltpu.VMEM((DIM, ROWS), bf16),
            pltpu.VMEM((3 * BLOCK, BLOCK), f32), pltpu.VMEM((3 * BLOCK, BLOCK), f32),
            pltpu.VMEM((3 * BLOCK, BLOCK), bf16), pltpu.VMEM((3 * BLOCK, BLOCK), bf16),
        ],
        limit=32,
    )
    edge = call(
        edges_kernel, [live, back, ahead, spectra, *halos],
        shape(DIM, 2 * BLOCK, bf16), 2 * per_block,
    )

    last = reps - 1
    away_pairs = [(d * reps, (d - 1) * reps) for d in range(1, bands)]
    away_pairs += [(d * reps + last, (d + 1) * reps + last) for d in range(bands - 1)]
    swaps = [
        [(d * reps + r, d * reps + partners(r, d & 1, reps)[step]) for d in range(bands) for r in range(reps)]
        for step in range(2)
    ]
    arrived = {role: lax.ppermute(sum_block(role, True), both, away_pairs) for role in (3, 1, 2, 0)}

    def exchanged(role, step, *more):
        own = sum_block(role, False)
        block = call(add_kernel, [own, arrived[role], *more], shape(CL_DEV, DIM, bf16), 1 << 20)
        return lax.ppermute(block, both, swaps[step])

    for_second = exchanged(3, 0)
    mine_first = exchanged(1, 0)
    mine_second = exchanged(2, 1, for_second)
    own = sum_block(0, False)
    return call(finish_kernel, [own, arrived[0], mine_first, mine_second], shape(CL_DEV, DIM, f32), 1 << 20)


def solution(mesh):
    rows = P(("mz", "rep"))

    return jax.shard_map(
        shards,
        mesh=mesh,
        in_specs=(P(("mz", "rep"), None), rows, rows, rows, rows),
        out_specs=P(("mz", "rep"), None),
        check_vma=False,
    )
```

```python
import functools

import jax
import jax.numpy as jnp
from jax import lax
from jax.experimental import pallas as pl
from jax.experimental.pallas import tpu as pltpu
from jax.sharding import PartitionSpec as P


DIM = 512
BLOCK = 256
CL_DEV = 512
ROWS = 4096
NBLK = ROWS // BLOCK
HALO = BLOCK + 16
FAR = -(1 << 24)
SCALE = 3.0 * 1.4426950408889634
f32, bf16, i32 = jnp.float32, jnp.bfloat16, jnp.int32
NT = (((1,), (1,)), ((), ()))


def unit_rows(block):
    values = block.astype(f32)
    square = jnp.sum(values * values, axis=1, keepdims=True)
    return (values * lax.rsqrt(square + 1e-06)).astype(bf16)


def transposed(unit):
    return jnp.transpose(unit)


def attend(query, back, ahead, cap, keys, keys_t, low_cap, high_cap, score_ref, weight_ref):
    at = lax.broadcasted_iota(i32, (1, BLOCK), 1) + BLOCK
    low = at - back
    high = at + ahead
    own = jnp.minimum(high, cap - 1)
    total = jnp.zeros((1, BLOCK), f32)
    score_ref[...] = lax.dot_general(keys, query, NT, preferred_element_type=f32)
    for k in range(3):
        span = slice(k * BLOCK, (k + 1) * BLOCK)
        slot = lax.broadcasted_iota(i32, (BLOCK, BLOCK), 0) + k * BLOCK
        if k == 0:
            keep = slot >= low
            if low_cap is not None:
                keep = keep & (slot < low_cap)
        elif k == 1:
            keep = ((slot >= low) & (slot <= own)) | (slot == at)
        elif high_cap is None:
            keep = slot <= own
        else:
            keep = slot <= jnp.minimum(high, high_cap - 1)
        weight = jnp.where(keep, jnp.exp2(score_ref[span, :] * SCALE - SCALE), 0.0)
        total = total + jnp.sum(weight, axis=0, keepdims=True)
        weight_ref[span, :] = weight.astype(bf16)
    mixed = jnp.dot(keys_t, weight_ref[...], preferred_element_type=f32)
    return (mixed * (1.0 / total)).astype(bf16)


def pack_kernel(live_ref, first_ref, last_ref, one_ref, two_ref):
    live = live_ref[0]
    row = lax.broadcasted_iota(i32, (HALO - BLOCK, DIM), 0)
    digits = jnp.where(row == 0, live >> 6, live & 63).astype(f32).astype(bf16)
    one_ref[BLOCK:, :] = digits
    two_ref[BLOCK:, :] = digits
    even = lax.axis_index("rep") % 2 == 0
    for is_even, one, two in ((True, last_ref, first_ref), (False, first_ref, last_ref)):

        @pl.when(even == is_even)
        def _():
            one_ref[:BLOCK, :] = one[...]
            two_ref[:BLOCK, :] = two[...]


def interior_kernel(
    live_ref, back_ref, ahead_ref, rows_ref, out_ref,
    unit_ref, unit_t_ref, score_a, score_b, weight_a, weight_b,
):
    live = live_ref[0]

    def block(index):
        return pl.ds(pl.multiple_of(index * BLOCK, BLOCK), BLOCK)

    def prepare(index):
        unit = unit_rows(rows_ref[block(index), :])
        unit_ref[block(index), :] = unit
        unit_t_ref[:, block(index)] = transposed(unit)

    def score(index, score_ref):
        keys = unit_ref[pl.ds(pl.multiple_of((index - 1) * BLOCK, BLOCK), 3 * BLOCK), :]
        score_ref[...] = lax.dot_general(keys, unit_ref[block(index), :], NT, preferred_element_type=f32)

    def finish(index, score_ref, weight_ref):
        at = lax.broadcasted_iota(i32, (1, BLOCK), 1) + BLOCK
        low = at - back_ref[:, block(index)]
        high = jnp.minimum(at + ahead_ref[:, block(index)], live - (index - 1) * BLOCK - 1)
        total = jnp.zeros((1, BLOCK), f32)
        for k in range(3):
            slot = lax.broadcasted_iota(i32, (BLOCK, BLOCK), 0) + k * BLOCK
            keep = (slot >= low, ((slot >= low) & (slot <= high)) | (slot == at), slot <= high)[k]
            span = slice(k * BLOCK, (k + 1) * BLOCK)
            weight = jnp.where(keep, jnp.exp2(score_ref[span, :] * SCALE - SCALE), 0.0)
            total = total + jnp.sum(weight, axis=0, keepdims=True)
            weight_ref[span, :] = weight.astype(bf16)
        keys_t = unit_t_ref[:, pl.ds(pl.multiple_of((index - 1) * BLOCK, BLOCK), 3 * BLOCK)]
        mixed = jnp.dot(keys_t, weight_ref[...], preferred_element_type=f32)
        out_ref[:, block(index - 1)] = (mixed * (1.0 / total)).astype(bf16)

    def early(index, _):
        prepare(index)
        return 0

    lax.fori_loop(0, 4, early, 0)
    score(1, score_a)

    def step(pair, _):
        index = 2 * pair + 1
        score(index + 1, score_b)
        finish(index, score_a, weight_a)
        prepare(jnp.minimum(index + 3, NBLK - 1))
        score(jnp.minimum(index + 2, NBLK - 2), score_a)
        finish(index + 1, score_b, weight_b)
        prepare(jnp.minimum(index + 4, NBLK - 1))
        return 0

    lax.fori_loop(0, (NBLK - 2) // 2, step, 0)


def edges_kernel(
    live_ref, back_ref, ahead_ref, spectra_ref, one_ref, two_ref, out_ref,
    keys_ref, keys_t_ref, score_a, score_b, weight_a, weight_b,
):
    live = live_ref[0]
    even = lax.axis_index("rep") % 2 == 0

    def count(ref):
        digits = ref[BLOCK : BLOCK + 8, :BLOCK].astype(f32)
        return (digits[0:1] * 64.0 + digits[1:2]).astype(i32)

    count_one, count_two = count(one_ref), count(two_ref)
    count_below = jnp.where(even, count_two, count_one)
    count_above = jnp.where(even, count_one, count_two)

    def rows(block):
        return spectra_ref[block * BLOCK : (block + 1) * BLOCK, :]

    slot = jnp.where(even, 5, 0)
    blocks = ((1, rows(0)), (2, rows(1)), (3, rows(NBLK - 2)), (4, rows(NBLK - 1)))
    for n, block in blocks + ((slot, one_ref[:BLOCK, :]), (5 - slot, two_ref[:BLOCK, :])):
        unit = unit_rows(block)
        span = pl.ds(n * BLOCK if isinstance(n, int) else pl.multiple_of(n * BLOCK, BLOCK), BLOCK)
        keys_ref[span, :] = unit
        keys_t_ref[:, span] = transposed(unit)
    side = 3 * BLOCK
    out_ref[:, :BLOCK] = attend(
        keys_ref[BLOCK : 2 * BLOCK, :], back_ref[:, :BLOCK], ahead_ref[:, :BLOCK], live + BLOCK,
        keys_ref[:side, :], keys_t_ref[:, :side], count_below - (ROWS - BLOCK), None, score_a, weight_a,
    )
    out_ref[:, BLOCK:] = attend(
        keys_ref[side + BLOCK : side + 2 * BLOCK, :], back_ref[:, ROWS - BLOCK :], ahead_ref[:, ROWS - BLOCK :],
        live - (ROWS - 2 * BLOCK), keys_ref[side:, :], keys_t_ref[:, side:], None, count_above + 2 * BLOCK,
        score_b, weight_b,
    )


INNER = ROWS - 2 * BLOCK
CHUNK = 512


def partners(rep, parity, rep_count):
    across = rep_count - 1 - rep
    beside = rep + 1 - 2 * (rep & 1)
    if isinstance(rep, int):
        return (beside, across) if parity else (across, beside)
    odd = parity == 1
    return jnp.where(odd, beside, across), jnp.where(odd, across, beside)


def sums_kernel(role, away, rep_count, live_ref, ids_ref, inner_ref, edge_ref, out_ref):
    rep = lax.axis_index("rep")
    band = lax.axis_index("mz")
    if away:
        band = band + jnp.where(rep == 0, -1, 1)
    one, two = partners(rep, band & 1, rep_count)
    owner = (rep, one, two, partners(one, band & 1, rep_count)[1])[role]
    first = band * (CL_DEV * rep_count) + owner * CL_DEV

    def work():
        live = live_ref[0]
        lane = lax.broadcasted_iota(i32, (1, BLOCK), 1)

        def added(pieces, rows):
            wanted = jnp.concatenate(
                [
                    jnp.where(lane + start < live, ids_ref[:, start : start + BLOCK], FAR)
                    for start in pieces
                ],
                axis=1,
            )
            cluster = lax.broadcasted_iota(i32, (CL_DEV, CHUNK), 0)
            hot = jnp.where(cluster == wanted - first, 1.0, 0.0).astype(bf16)
            return lax.dot_general(hot, rows, NT, preferred_element_type=f32)

        acc = added((0, ROWS - BLOCK), edge_ref[...])
        for start in range(0, INNER, CHUNK):
            pieces = range(start + BLOCK, start + BLOCK + CHUNK, BLOCK)
            acc = acc + added(pieces, inner_ref[:, start : start + CHUNK])
        out_ref[...] = acc.astype(out_ref.dtype)

    if away:
        pl.when((rep == 0) | (rep == rep_count - 1))(work)
    else:
        work()


def add_kernel(own_ref, *rest):
    total = own_ref[...]
    for ref in rest[:-1]:
        total = total + ref[...].astype(f32)
    rest[-1][...] = total.astype(bf16)


PIECES = 4


def finish_kernel(own_ref, *rest):
    *parts, out_hbm, done_ref, sems = rest
    rows = CL_DEV // PIECES
    copies = []
    for n in range(PIECES):
        span = slice(n * rows, (n + 1) * rows)
        owned = own_ref[span, :]
        for ref in parts:
            owned = owned + ref[span, :].astype(f32)
        mean = jnp.sum(owned * owned, axis=1, keepdims=True) * (1.0 / DIM)
        done_ref[span, :] = owned / jnp.sqrt(mean + 1e-06)
        copies.append(pltpu.make_async_copy(done_ref.at[pl.ds(n * rows, rows)], out_hbm.at[pl.ds(n * rows, rows)], sems.at[n]))
        copies[-1].start()
    for copy in copies:
        copy.wait()


VMEM = pl.BlockSpec(memory_space=pltpu.VMEM)
SMEM = pl.BlockSpec(memory_space=pltpu.SMEM)
FARREF = pl.BlockSpec(memory_space=pltpu.HBM)
MIB = 1024 * 1024


def call(kernel, inputs, out_shape, flops, scratch=(), far_out=False, limit=16):
    one = not isinstance(out_shape, (list, tuple))
    in_specs = [
        SMEM if x.dtype == i32 and x.size < 64 else VMEM for x in inputs
    ]
    moved = sum(x.size * x.dtype.itemsize for x in inputs)
    return pl.pallas_call(
        kernel,
        out_shape=out_shape,
        in_specs=in_specs,
        out_specs=FARREF if far_out else VMEM if one else [VMEM] * len(out_shape),
        scratch_shapes=list(scratch),
        cost_estimate=pl.CostEstimate(flops=flops, bytes_accessed=moved, transcendentals=0),
        compiler_params=pltpu.CompilerParams(vmem_limit_bytes=limit * MIB),
    )(*inputs)


def shape(rows, columns, dtype):
    return jax.ShapeDtypeStruct((rows, columns), dtype)


def shards(spectra, reach_back, reach_ahead, live, cluster_ids):
    bands, reps = lax.axis_size("mz"), lax.axis_size("rep")
    every = bands * reps
    both = ("mz", "rep")

    def sum_block(role, away):
        return call(
            functools.partial(sums_kernel, role, away, reps), [live, ids, inner, edge],
            shape(CL_DEV, DIM, bf16 if away else f32), 2 * CL_DEV * ROWS * DIM,
        )

    back, ahead, ids = (x.reshape(1, ROWS) for x in (reach_back, reach_ahead, cluster_ids))
    blocks = call(
        pack_kernel, [live, spectra[:BLOCK], spectra[ROWS - BLOCK :]],
        [shape(HALO, DIM, bf16)] * 2, 1 << 33, limit=2,
    )
    pairs = [(i, i + 1) for i in range(every - 1)]
    halos = [
        lax.ppermute(block, both, sorted(pair[::way] for pair in pairs[turn::2] for way in (1, -1)))
        for turn, block in enumerate(blocks)
    ]
    per_block = 4 * BLOCK * 3 * BLOCK * DIM
    inner = call(
        interior_kernel, [live, back, ahead, spectra], shape(DIM, INNER, bf16), per_block * (NBLK - 2),
        [
            pltpu.VMEM((ROWS, DIM), bf16), pltpu.VMEM((DIM, ROWS), bf16),
            pltpu.VMEM((3 * BLOCK, BLOCK), f32), pltpu.VMEM((3 * BLOCK, BLOCK), f32),
            pltpu.VMEM((3 * BLOCK, BLOCK), bf16), pltpu.VMEM((3 * BLOCK, BLOCK), bf16),
        ],
        limit=32,
    )
    edge = call(
        edges_kernel, [live, back, ahead, spectra, *halos],
        shape(DIM, 2 * BLOCK, bf16), 2 * per_block,
        [
            pltpu.VMEM((6 * BLOCK, DIM), bf16), pltpu.VMEM((DIM, 6 * BLOCK), bf16),
            pltpu.VMEM((3 * BLOCK, BLOCK), f32), pltpu.VMEM((3 * BLOCK, BLOCK), f32),
            pltpu.VMEM((3 * BLOCK, BLOCK), bf16), pltpu.VMEM((3 * BLOCK, BLOCK), bf16),
        ],
    )

    last = reps - 1
    away_pairs = [(d * reps, (d - 1) * reps) for d in range(1, bands)]
    away_pairs += [(d * reps + last, (d + 1) * reps + last) for d in range(bands - 1)]
    swaps = [
        [(d * reps + r, d * reps + partners(r, d & 1, reps)[step]) for d in range(bands) for r in range(reps)]
        for step in range(2)
    ]
    arrived = {role: lax.ppermute(sum_block(role, True), both, away_pairs) for role in (3, 1, 2, 0)}

    def exchanged(role, step, *more):
        own = sum_block(role, False)
        block = call(add_kernel, [own, arrived[role], *more], shape(CL_DEV, DIM, bf16), 1 << 20)
        return lax.ppermute(block, both, swaps[step])

    for_second = exchanged(3, 0)
    mine_first = exchanged(1, 0)
    mine_second = exchanged(2, 1, for_second)
    own = sum_block(0, False)
    return call(
        finish_kernel, [own, arrived[0], mine_first, mine_second], shape(CL_DEV, DIM, f32), 1 << 20,
        [pltpu.VMEM((CL_DEV, DIM), f32), pltpu.SemaphoreType.DMA((PIECES,))], far_out=True,
    )


def solution(mesh):
    rows = P(("mz", "rep"))

    return jax.shard_map(
        shards,
        mesh=mesh,
        in_specs=(P(("mz", "rep"), None), rows, rows, rows, rows),
        out_specs=P(("mz", "rep"), None),
        check_vma=False,
    )
```

```python
import functools

import jax
import jax.numpy as jnp
from jax import lax
from jax.experimental import pallas as pl
from jax.experimental.pallas import tpu as pltpu
from jax.sharding import PartitionSpec as P


DIM = 512
BLOCK = 256
CL_DEV = 512
ROWS = 4096
NBLK = ROWS // BLOCK
HALO = BLOCK + 16
FAR = -(1 << 24)
SCALE = 3.0 * 1.4426950408889634
f32, bf16, i32 = jnp.float32, jnp.bfloat16, jnp.int32
NT = (((1,), (1,)), ((), ()))


def unit_rows(block):
    values = block.astype(f32)
    square = jnp.sum(values * values, axis=1, keepdims=True)
    return (values * lax.rsqrt(square + 1e-06)).astype(bf16)


def transposed(unit):
    return jnp.transpose(unit)


def attend(query, back, ahead, cap, keys, keys_t, low_cap, high_cap, score_ref, weight_ref):
    at = lax.broadcasted_iota(i32, (1, BLOCK), 1) + BLOCK
    low = at - back
    high = at + ahead
    own = jnp.minimum(high, cap - 1)
    total = jnp.zeros((1, BLOCK), f32)
    score_ref[...] = lax.dot_general(keys, query, NT, preferred_element_type=f32)
    for k in range(3):
        span = slice(k * BLOCK, (k + 1) * BLOCK)
        slot = lax.broadcasted_iota(i32, (BLOCK, BLOCK), 0) + k * BLOCK
        if k == 0:
            keep = slot >= low
            if low_cap is not None:
                keep = keep & (slot < low_cap)
        elif k == 1:
            keep = ((slot >= low) & (slot <= own)) | (slot == at)
        elif high_cap is None:
            keep = slot <= own
        else:
            keep = slot <= jnp.minimum(high, high_cap - 1)
        weight = jnp.where(keep, jnp.exp2(score_ref[span, :] * SCALE - SCALE), 0.0)
        total = total + jnp.sum(weight, axis=0, keepdims=True)
        weight_ref[span, :] = weight.astype(bf16)
    mixed = jnp.dot(keys_t, weight_ref[...], preferred_element_type=f32)
    return (mixed * (1.0 / total)).astype(bf16)


def pack_kernel(live_ref, first_ref, last_ref, one_ref, two_ref):
    live = live_ref[0]
    row = lax.broadcasted_iota(i32, (HALO - BLOCK, DIM), 0)
    digits = jnp.where(row == 0, live >> 6, live & 63).astype(f32).astype(bf16)
    one_ref[BLOCK:, :] = digits
    two_ref[BLOCK:, :] = digits
    even = lax.axis_index("rep") % 2 == 0
    for is_even, one, two in ((True, first_ref, last_ref), (False, last_ref, first_ref)):

        @pl.when(even == is_even)
        def _():
            one_ref[:BLOCK, :] = one[...]
            two_ref[:BLOCK, :] = two[...]


def interior_kernel(
    live_ref, back_ref, ahead_ref, rows_ref, out_ref,
    unit_ref, unit_t_ref, score_a, score_b, weight_a, weight_b,
):
    live = live_ref[0]

    def block(index):
        return pl.ds(pl.multiple_of(index * BLOCK, BLOCK), BLOCK)

    def prepare(index):
        unit = unit_rows(rows_ref[block(index), :])
        unit_ref[block(index), :] = unit
        unit_t_ref[:, block(index)] = transposed(unit)

    def score(index, score_ref):
        keys = unit_ref[pl.ds(pl.multiple_of((index - 1) * BLOCK, BLOCK), 3 * BLOCK), :]
        score_ref[...] = lax.dot_general(keys, unit_ref[block(index), :], NT, preferred_element_type=f32)

    def finish(index, score_ref, weight_ref):
        at = lax.broadcasted_iota(i32, (1, BLOCK), 1) + BLOCK
        low = at - back_ref[:, block(index)]
        high = jnp.minimum(at + ahead_ref[:, block(index)], live - (index - 1) * BLOCK - 1)
        total = jnp.zeros((1, BLOCK), f32)
        for k in range(3):
            slot = lax.broadcasted_iota(i32, (BLOCK, BLOCK), 0) + k * BLOCK
            keep = (slot >= low, ((slot >= low) & (slot <= high)) | (slot == at), slot <= high)[k]
            span = slice(k * BLOCK, (k + 1) * BLOCK)
            weight = jnp.where(keep, jnp.exp2(score_ref[span, :] * SCALE - SCALE), 0.0)
            total = total + jnp.sum(weight, axis=0, keepdims=True)
            weight_ref[span, :] = weight.astype(bf16)
        keys_t = unit_t_ref[:, pl.ds(pl.multiple_of((index - 1) * BLOCK, BLOCK), 3 * BLOCK)]
        mixed = jnp.dot(keys_t, weight_ref[...], preferred_element_type=f32)
        out_ref[:, block(index - 1)] = (mixed * (1.0 / total)).astype(bf16)

    def early(index, _):
        prepare(index)
        return 0

    lax.fori_loop(0, 4, early, 0)
    score(1, score_a)

    def step(pair, _):
        index = 2 * pair + 1
        score(index + 1, score_b)
        finish(index, score_a, weight_a)
        prepare(jnp.minimum(index + 3, NBLK - 1))
        score(jnp.minimum(index + 2, NBLK - 2), score_a)
        finish(index + 1, score_b, weight_b)
        prepare(jnp.minimum(index + 4, NBLK - 1))
        return 0

    lax.fori_loop(0, (NBLK - 2) // 2, step, 0)


def edges_kernel(
    live_ref, back_ref, ahead_ref, spectra_ref, one_ref, two_ref, out_ref,
    keys_ref, keys_t_ref, score_a, score_b, weight_a, weight_b,
):
    live = live_ref[0]
    even = lax.axis_index("rep") % 2 == 0

    def count(ref):
        digits = ref[BLOCK : BLOCK + 8, :BLOCK].astype(f32)
        return (digits[0:1] * 64.0 + digits[1:2]).astype(i32)

    count_one, count_two = count(one_ref), count(two_ref)
    count_below = jnp.where(even, count_one, count_two)
    count_above = jnp.where(even, count_two, count_one)

    def rows(block):
        return spectra_ref[block * BLOCK : (block + 1) * BLOCK, :]

    slot = jnp.where(even, 0, 5)
    blocks = ((1, rows(0)), (2, rows(1)), (3, rows(NBLK - 2)), (4, rows(NBLK - 1)))
    for n, block in blocks + ((slot, one_ref[:BLOCK, :]), (5 - slot, two_ref[:BLOCK, :])):
        unit = unit_rows(block)
        span = pl.ds(n * BLOCK if isinstance(n, int) else pl.multiple_of(n * BLOCK, BLOCK), BLOCK)
        keys_ref[span, :] = unit
        keys_t_ref[:, span] = transposed(unit)
    side = 3 * BLOCK
    out_ref[:, :BLOCK] = attend(
        keys_ref[BLOCK : 2 * BLOCK, :], back_ref[:, :BLOCK], ahead_ref[:, :BLOCK], live + BLOCK,
        keys_ref[:side, :], keys_t_ref[:, :side], count_below - (ROWS - BLOCK), None, score_a, weight_a,
    )
    out_ref[:, BLOCK:] = attend(
        keys_ref[side + BLOCK : side + 2 * BLOCK, :], back_ref[:, ROWS - BLOCK :], ahead_ref[:, ROWS - BLOCK :],
        live - (ROWS - 2 * BLOCK), keys_ref[side:, :], keys_t_ref[:, side:], None, count_above + 2 * BLOCK,
        score_b, weight_b,
    )


INNER = ROWS - 2 * BLOCK
CHUNK = 1792


def partners(rep, parity, rep_count):
    across = rep_count - 1 - rep
    beside = rep + 1 - 2 * (rep & 1)
    if isinstance(rep, int):
        return (beside, across) if parity else (across, beside)
    odd = parity == 1
    return jnp.where(odd, beside, across), jnp.where(odd, across, beside)


def sums_kernel(role, away, rep_count, live_ref, ids_ref, inner_ref, edge_ref, out_ref):
    rep = lax.axis_index("rep")
    band = lax.axis_index("mz")
    if away:
        band = band + jnp.where(rep == 0, -1, 1)
    one, two = partners(rep, band & 1, rep_count)
    owner = (rep, one, two, partners(one, band & 1, rep_count)[1])[role]
    first = band * (CL_DEV * rep_count) + owner * CL_DEV

    def work():
        live = live_ref[0]
        lane = lax.broadcasted_iota(i32, (1, BLOCK), 1)

        def added(pieces, rows):
            wanted = jnp.concatenate(
                [
                    jnp.where(lane + start < live, ids_ref[:, start : start + BLOCK], FAR)
                    for start in pieces
                ],
                axis=1,
            )
            cluster = lax.broadcasted_iota(i32, (CL_DEV, rows.shape[1]), 0)
            hot = jnp.where(cluster == wanted - first, 1.0, 0.0).astype(bf16)
            return lax.dot_general(hot, rows, NT, preferred_element_type=f32)

        acc = added((0, ROWS - BLOCK), edge_ref[...])
        for start in range(0, INNER, CHUNK):
            pieces = range(start + BLOCK, start + BLOCK + CHUNK, BLOCK)
            acc = acc + added(pieces, inner_ref[:, start : start + CHUNK])
        out_ref[...] = acc.astype(out_ref.dtype)

    if away:
        pl.when((rep == 0) | (rep == rep_count - 1))(work)
    else:
        work()


def add_kernel(own_ref, *rest):
    total = own_ref[...]
    for ref in rest[:-1]:
        total = total + ref[...].astype(f32)
    rest[-1][...] = total.astype(bf16)


PIECES = 4


def finish_kernel(own_ref, *rest):
    *parts, out_hbm, done_ref, sems = rest
    rows = CL_DEV // PIECES
    copies = []
    for n in range(PIECES):
        span = slice(n * rows, (n + 1) * rows)
        owned = own_ref[span, :]
        for ref in parts:
            owned = owned + ref[span, :].astype(f32)
        mean = jnp.sum(owned * owned, axis=1, keepdims=True) * (1.0 / DIM)
        done_ref[span, :] = owned / jnp.sqrt(mean + 1e-06)
        copies.append(pltpu.make_async_copy(done_ref.at[pl.ds(n * rows, rows)], out_hbm.at[pl.ds(n * rows, rows)], sems.at[n]))
        copies[-1].start()
    for copy in copies:
        copy.wait()


VMEM = pl.BlockSpec(memory_space=pltpu.VMEM)
SMEM = pl.BlockSpec(memory_space=pltpu.SMEM)
FARREF = pl.BlockSpec(memory_space=pltpu.HBM)
MIB = 1024 * 1024


def call(kernel, inputs, out_shape, flops, scratch=(), far_out=False, limit=16):
    one = not isinstance(out_shape, (list, tuple))
    in_specs = [
        SMEM if x.dtype == i32 and x.size < 64 else VMEM for x in inputs
    ]
    moved = sum(x.size * x.dtype.itemsize for x in inputs)
    return pl.pallas_call(
        kernel,
        out_shape=out_shape,
        in_specs=in_specs,
        out_specs=FARREF if far_out else VMEM if one else [VMEM] * len(out_shape),
        scratch_shapes=list(scratch),
        cost_estimate=pl.CostEstimate(flops=flops, bytes_accessed=moved, transcendentals=0),
        compiler_params=pltpu.CompilerParams(vmem_limit_bytes=limit * MIB),
    )(*inputs)


def shape(rows, columns, dtype):
    return jax.ShapeDtypeStruct((rows, columns), dtype)


def shards(spectra, reach_back, reach_ahead, live, cluster_ids):
    bands, reps = lax.axis_size("mz"), lax.axis_size("rep")
    every = bands * reps
    both = ("mz", "rep")

    def sum_block(role, away):
        return call(
            functools.partial(sums_kernel, role, away, reps), [live, ids, inner, edge],
            shape(CL_DEV, DIM, bf16 if away else f32), 2 * CL_DEV * ROWS * DIM,
        )

    back, ahead, ids = (x.reshape(1, ROWS) for x in (reach_back, reach_ahead, cluster_ids))
    blocks = call(
        pack_kernel, [live, spectra[:BLOCK], spectra[ROWS - BLOCK :]],
        [shape(HALO, DIM, bf16)] * 2, 1 << 33, limit=2,
    )
    pairs = [(i, i + 1) for i in range(every - 1)]
    halos = [
        lax.ppermute(block, both, sorted(pair[::way] for pair in pairs[1 - turn :: 2] for way in (1, -1)))
        for turn, block in enumerate(blocks)
    ]
    per_block = 4 * BLOCK * 3 * BLOCK * DIM
    inner = call(
        interior_kernel, [live, back, ahead, spectra], shape(DIM, INNER, bf16), per_block * (NBLK - 2),
        [
            pltpu.VMEM((ROWS, DIM), bf16), pltpu.VMEM((DIM, ROWS), bf16),
            pltpu.VMEM((3 * BLOCK, BLOCK), f32), pltpu.VMEM((3 * BLOCK, BLOCK), f32),
            pltpu.VMEM((3 * BLOCK, BLOCK), bf16), pltpu.VMEM((3 * BLOCK, BLOCK), bf16),
        ],
        limit=32,
    )
    edge = call(
        edges_kernel, [live, back, ahead, spectra, *halos],
        shape(DIM, 2 * BLOCK, bf16), 2 * per_block,
        [
            pltpu.VMEM((6 * BLOCK, DIM), bf16), pltpu.VMEM((DIM, 6 * BLOCK), bf16),
            pltpu.VMEM((3 * BLOCK, BLOCK), f32), pltpu.VMEM((3 * BLOCK, BLOCK), f32),
            pltpu.VMEM((3 * BLOCK, BLOCK), bf16), pltpu.VMEM((3 * BLOCK, BLOCK), bf16),
        ],
    )

    last = reps - 1
    away_pairs = [(d * reps, (d - 1) * reps) for d in range(1, bands)]
    away_pairs += [(d * reps + last, (d + 1) * reps + last) for d in range(bands - 1)]
    swaps = [
        [(d * reps + r, d * reps + partners(r, d & 1, reps)[step]) for d in range(bands) for r in range(reps)]
        for step in range(2)
    ]
    arrived = {role: lax.ppermute(sum_block(role, True), both, away_pairs) for role in (3, 1, 2, 0)}

    def exchanged(role, step, *more):
        own = sum_block(role, False)
        block = call(add_kernel, [own, arrived[role], *more], shape(CL_DEV, DIM, bf16), 1 << 20)
        return lax.ppermute(block, both, swaps[step])

    for_second = exchanged(3, 0)
    mine_first = exchanged(1, 0)
    mine_second = exchanged(2, 1, for_second)
    own = sum_block(0, False)
    return call(
        finish_kernel, [own, arrived[0], mine_first, mine_second], shape(CL_DEV, DIM, f32), 1 << 20,
        [pltpu.VMEM((CL_DEV, DIM), f32), pltpu.SemaphoreType.DMA((PIECES,))], far_out=True,
    )


def solution(mesh):
    rows = P(("mz", "rep"))

    return jax.shard_map(
        shards,
        mesh=mesh,
        in_specs=(P(("mz", "rep"), None), rows, rows, rows, rows),
        out_specs=P(("mz", "rep"), None),
        check_vma=False,
    )
```
